128 devices in a mesh: ty: 8 (over y_hi, x), tx: 16 (over y_lo, z, core).
Axes of the slice: x: 4, y: 4 (y_hi: 2, y_lo: 2; y = y_hi * 2 + y_lo), z: 4, core: 2. Of those that a mesh axis runs over, the one named last changes fastest.
Arguments:
- surface_levels: float32 [1024, 32768], P('ty', 'tx'), may hold values from -6 to 6
- bearing_index: int32 [4], replicated, may hold values from 0 to 15
- stencil_displacements: int32 [4], replicated, may hold values from -4 to 4
- camera_altitude_class: int32 [4], replicated, may hold values from 0 to 3
Outputs:
- margin: float32 [4, 1024, 32768], P(None, 'ty', 'tx')
The draws below stay inside these ranges and needn't reach their ends.
Inputs may be any that keep to these rules, and one draw needn't show every extreme that they name: `bearing_index`: azimuth indices.
All inputs are finite; a program needn't handle non-finite values.
Results may differ from the reference program's by a relative error of at most 0.00002.
Values sent between devices are 32-bit elements; how exact they have to be, the bound alone decides.
A program may use at most 192 MiB of HBM per device.

```python
import math
import jax
import jax.numpy as jnp
from jax import lax

AZIMUTHS = 4
STENCIL_REACH = 4
GRID_LENGTH = 1024
GRID_WIDTH = 32768


def place_ends(result, stream_key, least, top_value):
    spot = [jax.random.randint(jax.random.fold_in(stream_key, axis), (), 0, length) for axis, length in enumerate(result.shape)]
    widest = result.shape.index(max(result.shape))
    beside = spot[:widest] + [(spot[widest] + 1) % result.shape[widest]] + spot[widest + 1:]
    return result.at[tuple(spot)].set(least).at[tuple(beside)].set(top_value)


def block_scale(stream_key, shape, shards, least, top_value):
    level = 1.0
    for axis_at, shards_of in shards:
        draws = jax.random.uniform(jax.random.fold_in(jax.random.fold_in(stream_key, 6), axis_at), (shards_of,), jnp.float32, least / len(shards), top_value / len(shards))
        level = level * jnp.repeat(jnp.exp(draws), shape[axis_at] // shards_of).reshape((-1,) + (1,) * (len(shape) - 1 - axis_at))
    return level


def scatter_about(own_key, dims, width, bound, pieces=(), held_as=jnp.bfloat16):
    result = width * jax.random.normal(own_key, dims, jnp.float32)
    if pieces:
        result = result * block_scale(own_key, dims, pieces, -0.22, 0.18)
    return jnp.clip(result, -bound, bound).astype(held_as)


def setup_inputs(seed: int = 0) -> dict:
    key_list = jax.random.split(jax.random.key(seed), 5)
    surface_levels = scatter_about(key_list[0], (GRID_LENGTH, GRID_WIDTH), 1.0, 6.0, ((0, 8), (1, 16)), jnp.float32)
    bearing_index = place_ends(jax.random.randint(key_list[1], (AZIMUTHS,), 0, 16), jax.random.fold_in(key_list[1], 1), 0, 15).astype(jnp.int32)
    stencil_displacements = place_ends(jax.random.randint(key_list[2], (AZIMUTHS,), -STENCIL_REACH, STENCIL_REACH + 1), jax.random.fold_in(key_list[2], 1), -STENCIL_REACH, STENCIL_REACH).astype(jnp.int32)
    camera_altitude_class = place_ends(jax.random.randint(key_list[3], (AZIMUTHS,), 0, 4), jax.random.fold_in(key_list[3], 1), 0, 3).astype(jnp.int32)
    return {"surface_levels": surface_levels, "bearing_index": bearing_index, "stencil_displacements": stencil_displacements, "camera_altitude_class": camera_altitude_class}


def view_tables(bearing_index, camera_altitude_class, easting_span):
    angle_idx = bearing_index.astype(jnp.float32)
    frac = (((bearing_index * 5) % 16).astype(jnp.float32) + 0.5) / 16.0
    theta = (angle_idx - 7.5) * (math.pi / 32.0)
    stride = 1.0 / jnp.cos(theta)
    slope = (1.0 + camera_altitude_class.astype(jnp.float32)) / (4.0 * easting_span)
    cube = frac * frac * frac
    square = frac * frac
    weights = jnp.stack([(-cube + 2.0 * square - frac) / 2.0, (3.0 * cube - 5.0 * square + 2.0) / 2.0, (-3.0 * cube + 4.0 * square + frac) / 2.0, (cube - square) / 2.0], axis=1)
    return weights, stride * slope


def reference(surface_levels, bearing_index, stencil_displacements, camera_altitude_class):
    northing_extent, easting_span = surface_levels.shape
    weights, rise = view_tables(bearing_index, camera_altitude_class, easting_span)
    border_lines = STENCIL_REACH + 2
    bordered_surface = jnp.pad(surface_levels, ((border_lines, border_lines), (0, 0)))
    columns = jnp.arange(easting_span).astype(jnp.float32)
    outputs = []
    for which in range(AZIMUTHS):
        strips = jnp.zeros((northing_extent, easting_span), jnp.float32)
        for tap_index in range(4):
            start = (stencil_displacements[which] + tap_index + STENCIL_REACH + 1).astype(jnp.int32)
            strips = strips + weights[which, tap_index] * lax.dynamic_slice_in_dim(bordered_surface, start, northing_extent, 0)
        lifted = strips + rise[which] * columns[None, :]
        running = lax.cummax(lifted, axis=1)
        lowest = jnp.full((northing_extent, 1), -jnp.inf, jnp.float32)
        horizon = jnp.concatenate([lowest, running[:, :-1]], axis=1)
        outputs.append(jnp.maximum(horizon - lifted, 0.0))
    return jnp.stack(outputs, axis=0)
```

```python
import functools
import math

import jax
import jax.numpy as jnp
from jax import lax
from jax.experimental import pallas as pl
from jax.experimental.pallas import tpu as pltpu
from jax.sharding import PartitionSpec as P

VIEWS = 4
ROWS = 128
LANES = 128
NEG = -jnp.inf


def tables(bearing, camera, k, span):
    a = jnp.full((8, LANES), bearing[k], jnp.int32)
    cls = jnp.full((8, LANES), camera[k], jnp.int32).astype(jnp.float32)
    f = (((a * 5) & 15).astype(jnp.float32) + 0.5) / 16.0
    theta = (a.astype(jnp.float32) - 7.5) * (math.pi / 32.0)
    stride = 1.0 / jnp.cos(theta)
    slope = (1.0 + cls) / (4.0 * span)
    cube = f * f * f
    square = f * f
    taps = (
        (-cube + 2.0 * square - f) / 2.0,
        (3.0 * cube - 5.0 * square + 2.0) / 2.0,
        (-3.0 * cube + 4.0 * square + f) / 2.0,
        (cube - square) / 2.0,
    )
    return taps, stride * slope


def kernel(
    nty, ntx, chunks, early,
    x_hbm, bearing_hbm, shift_hbm, camera_hbm, out,
    bearing, shift, camera, xs, top, bot, ls, wv, peaks, bpeaks, msg_i, msg_b, in_i, in_b, bsplat_i, bsplat_b,
    in_sem, tab_sem, halo_send, halo_recv, pre_send_i, pre_recv_i, pre_send_b, pre_recv_b,
):
    ty = lax.axis_index("ty")
    tx = lax.axis_index("tx")
    width = chunks * LANES
    span = width * ntx
    has_up = ty > 0
    has_down = ty < nty - 1

    in_i[...] = jnp.full(in_i.shape, NEG, jnp.float32)
    in_b[...] = jnp.full(in_b.shape, NEG, jnp.float32)

    loads = [
        pltpu.make_async_copy(
            x_hbm.at[:, pl.ds(c * LANES, LANES)], xs.at[c], in_sem.at[c]
        )
        for c in range(chunks)
    ]
    small = [
        pltpu.make_async_copy(src, dst, tab_sem.at[n])
        for n, (src, dst) in enumerate(
            ((bearing_hbm, bearing), (shift_hbm, shift), (camera_hbm, camera))
        )
    ]
    for copy in small + loads:
        copy.start()

    barrier = pltpu.get_barrier_semaphore()

    def greet(p):
        pl.semaphore_signal(barrier, inc=1, device_id=p, device_id_type=pl.DeviceIdType.MESH)

    @pl.when(has_up)
    def _():
        greet({"ty": ty - 1, "tx": tx})

    @pl.when(has_down)
    def _():
        greet({"ty": ty + 1, "tx": tx})

    for p in range(ntx):
        @pl.when(p < tx)
        def _():
            greet({"ty": ty, "tx": p})

    for copy in small:
        copy.wait()

    for k in range(VIEWS):
        taps, rise = tables(bearing, camera, k, span)
        for j in range(4):
            wv[k, j] = taps[j]
        wv[k, 4] = rise

    for copy in loads:
        copy.wait()
    for c in range(chunks):
        top[c, 8:24] = xs[c, 0:16]
        bot[c, 0:16] = xs[c, ROWS - 16:ROWS]

    @pl.when(jnp.logical_not(has_up))
    def _():
        for c in range(chunks):
            top[c, 0:8] = jnp.zeros((8, LANES), jnp.float32)

    @pl.when(jnp.logical_not(has_down))
    def _():
        for c in range(chunks):
            bot[c, 16:24] = jnp.zeros((8, LANES), jnp.float32)

    lane = lax.broadcasted_iota(jnp.int32, (8, LANES), 1)
    first = tx * width

    def tile_scan(src, base, row, want_peak):
        result = []
        for k in range(VIEWS):
            w = [wv[k, j] for j in range(4)]
            rise = wv[k, 4]
            start = base + shift[k]
            carry = None
            for c in range(chunks):
                acc = w[0] * src[c, pl.ds(start - 1, 8), :]
                for j in range(1, 4):
                    acc = acc + w[j] * src[c, pl.ds(start + j - 1, 8), :]
                cols = (lane + (first + c * LANES)).astype(jnp.float32)
                lifted = acc + rise * cols
                ls[k, pl.ds(row, 8), pl.ds(c * LANES, LANES)] = lifted
                run = lifted
                step = 1
                while step < LANES:
                    run = jnp.maximum(run, jnp.where(lane >= step, pltpu.roll(run, step, 1), NEG))
                    step *= 2
                if carry is not None:
                    run = jnp.maximum(run, carry)
                out[k, pl.ds(row, 8), pl.ds(c * LANES, LANES)] = run
                carry = jnp.broadcast_to(run[:, LANES - 1:LANES], (8, LANES))
            result.append(carry)
        return result

    def interior(i, _):
        row = pl.multiple_of(i * 8, 8)
        for k, peak in enumerate(tile_scan(xs, row, row, True)):
            peaks[k, pl.ds(row, 8), :] = peak
        return 0

    for k in range(VIEWS):
        peaks[k, 0:8, :] = jnp.full((8, LANES), NEG, jnp.float32)
        peaks[k, ROWS - 8:ROWS, :] = jnp.full((8, LANES), NEG, jnp.float32)

    tiles = ROWS // 8
    lax.fori_loop(1, 1 + early, interior, 0)

    waits = (ntx - 1 - tx) + has_up.astype(jnp.int32) + has_down.astype(jnp.int32)
    pl.semaphore_wait(barrier, waits)

    up = pltpu.make_async_remote_copy(
        src_ref=xs.at[:, pl.ds(0, 8), :], dst_ref=bot.at[:, pl.ds(16, 8), :],
        send_sem=halo_send.at[0], recv_sem=halo_recv.at[0],
        device_id={"ty": ty - 1, "tx": tx}, device_id_type=pl.DeviceIdType.MESH,
    )
    down = pltpu.make_async_remote_copy(
        src_ref=xs.at[:, pl.ds(ROWS - 8, 8), :], dst_ref=top.at[:, pl.ds(0, 8), :],
        send_sem=halo_send.at[1], recv_sem=halo_recv.at[1],
        device_id={"ty": ty + 1, "tx": tx}, device_id_type=pl.DeviceIdType.MESH,
    )

    @pl.when(has_up)
    def _():
        up.start()

    @pl.when(has_down)
    def _():
        down.start()

    lax.fori_loop(1 + early, tiles - 1, interior, 0)

    def spread(msg, store, send, recv):
        copies = {
            p: pltpu.make_async_remote_copy(
                src_ref=msg, dst_ref=store.at[tx], send_sem=send.at[p], recv_sem=recv.at[tx],
                device_id={"ty": ty, "tx": p}, device_id_type=pl.DeviceIdType.MESH,
            )
            for p in range(1, ntx)
        }
        for p in range(1, ntx):
            @pl.when(p > tx)
            def _():
                copies[p].start()
        return copies

    def finish_sends(copies):
        for p in range(1, ntx):
            @pl.when(p > tx)
            def _():
                copies[p].wait_send()

    def receive(msg, store, recv):
        for p in range(ntx - 1):
            @pl.when(p < tx)
            def _():
                pltpu.make_async_remote_copy(
                    src_ref=msg, dst_ref=store.at[p], send_sem=recv.at[p], recv_sem=recv.at[p],
                    device_id={"ty": ty, "tx": p}, device_id_type=pl.DeviceIdType.MESH,
                ).wait_recv()

    for k in range(VIEWS):
        msg_i[k] = jnp.max(peaks[k].T, axis=0, keepdims=True)
    sent_i = spread(msg_i, in_i, pre_send_i, pre_recv_i)

    @pl.when(has_down)
    def _():
        up_in = pltpu.make_async_remote_copy(
            src_ref=xs.at[:, pl.ds(0, 8), :], dst_ref=bot.at[:, pl.ds(16, 8), :],
            send_sem=halo_send.at[0], recv_sem=halo_recv.at[0],
            device_id={"ty": ty + 1, "tx": tx}, device_id_type=pl.DeviceIdType.MESH,
        )
        up_in.wait_recv()

    @pl.when(has_up)
    def _():
        down_in = pltpu.make_async_remote_copy(
            src_ref=xs.at[:, pl.ds(ROWS - 8, 8), :], dst_ref=top.at[:, pl.ds(0, 8), :],
            send_sem=halo_send.at[1], recv_sem=halo_recv.at[1],
            device_id={"ty": ty - 1, "tx": tx}, device_id_type=pl.DeviceIdType.MESH,
        )
        down_in.wait_recv()

    bpeaks[...] = jnp.full(bpeaks.shape, NEG, jnp.float32)
    for k, peak in enumerate(tile_scan(top, 8, 0, True)):
        bpeaks[16 * k:16 * k + 8, :] = peak
    for k, peak in enumerate(tile_scan(bot, 8, ROWS - 8, True)):
        bpeaks[16 * k + 8:16 * k + 16, :] = peak
    msg_b[...] = jnp.max(bpeaks[...].T, axis=0, keepdims=True)
    sent_b = spread(msg_b, in_b, pre_send_b, pre_recv_b)

    receive(msg_i, in_i, pre_recv_i)
    for k in range(VIEWS):
        best = in_i[0, k]
        for p in range(1, ntx):
            best = jnp.maximum(best, in_i[p, k])
        bsplat_i[k] = jnp.broadcast_to(best, (LANES, LANES)).T

    def close(k, row, before):
        for c in range(chunks):
            at = (k, pl.ds(row, 8), pl.ds(c * LANES, LANES))
            out[at] = jnp.maximum(out[at], before) - ls[at]

    def close_interior(i, _):
        row = pl.multiple_of(i * 8, 8)
        for k in range(VIEWS):
            close(k, row, bsplat_i[k, pl.ds(row, 8), :])
        return 0

    lax.fori_loop(1, tiles - 1, close_interior, 0)

    receive(msg_b, in_b, pre_recv_b)
    best = in_b[0]
    for p in range(1, ntx):
        best = jnp.maximum(best, in_b[p])
    bsplat_b[...] = jnp.broadcast_to(best, (LANES, LANES)).T
    for k in range(VIEWS):
        close(k, 0, bsplat_b[16 * k:16 * k + 8, :])
        close(k, ROWS - 8, bsplat_b[16 * k + 8:16 * k + 16, :])

    @pl.when(has_up)
    def _():
        up.wait_send()

    @pl.when(has_down)
    def _():
        down.wait_send()

    finish_sends(sent_i)
    finish_sends(sent_b)


def on_device(surface_levels, bearing_index, stencil_displacements, camera_altitude_class):
    rows, width = surface_levels.shape
    nty, ntx = lax.axis_size("ty"), lax.axis_size("tx")
    chunks = width // LANES
    vm = lambda *s: pltpu.VMEM(s, jnp.float32)
    return pl.pallas_call(
        functools.partial(kernel, nty, ntx, chunks, 4),
        out_shape=jax.ShapeDtypeStruct((VIEWS, rows, width), jnp.float32),
        in_specs=[pl.BlockSpec(memory_space=pltpu.HBM)] * 4,
        out_specs=pl.BlockSpec(memory_space=pltpu.VMEM),
        scratch_shapes=[
            pltpu.SMEM((VIEWS,), jnp.int32), pltpu.SMEM((VIEWS,), jnp.int32),
            pltpu.SMEM((VIEWS,), jnp.int32),
            vm(chunks, ROWS, LANES), vm(chunks, 24, LANES), vm(chunks, 24, LANES),
            vm(VIEWS, rows, width), vm(VIEWS, 5, 8, LANES),
            vm(VIEWS, ROWS, LANES), vm(LANES, LANES),
            vm(VIEWS, 1, LANES), vm(1, LANES),
            vm(ntx, VIEWS, 1, LANES), vm(ntx, 1, LANES),
            vm(VIEWS, LANES, LANES), vm(LANES, LANES),
            pltpu.SemaphoreType.DMA((chunks,)),
            pltpu.SemaphoreType.DMA((3,)),
            pltpu.SemaphoreType.DMA((2,)), pltpu.SemaphoreType.DMA((2,)),
            pltpu.SemaphoreType.DMA((ntx,)), pltpu.SemaphoreType.DMA((ntx,)),
            pltpu.SemaphoreType.DMA((ntx,)), pltpu.SemaphoreType.DMA((ntx,)),
        ],
        compiler_params=pltpu.CompilerParams(
            collective_id=0, has_side_effects=True, vmem_limit_bytes=40 * 1024 * 1024
        ),
        name="horizon",
    )(surface_levels, bearing_index, stencil_displacements, camera_altitude_class)


def solution(mesh):
    return jax.shard_map(
        on_device,
        mesh=mesh,
        in_specs=(P("ty", "tx"), P(), P(), P()),
        out_specs=P(None, "ty", "tx"),
        check_vma=False,
    )
```

```python
import functools
import math

import jax
import jax.numpy as jnp
from jax import lax
from jax.experimental import pallas as pl
from jax.experimental.pallas import tpu as pltpu
from jax.sharding import PartitionSpec as P

VIEWS = 4
ROWS = 128
LANES = 128
NEG = -jnp.inf


def tables(bearing, camera, k, span):
    a = jnp.full((8, LANES), bearing[k], jnp.int32)
    cls = jnp.full((8, LANES), camera[k], jnp.int32).astype(jnp.float32)
    f = (((a * 5) & 15).astype(jnp.float32) + 0.5) / 16.0
    theta = (a.astype(jnp.float32) - 7.5) * (math.pi / 32.0)
    stride = 1.0 / jnp.cos(theta)
    slope = (1.0 + cls) / (4.0 * span)
    cube = f * f * f
    square = f * f
    taps = (
        (-cube + 2.0 * square - f) / 2.0,
        (3.0 * cube - 5.0 * square + 2.0) / 2.0,
        (-3.0 * cube + 4.0 * square + f) / 2.0,
        (cube - square) / 2.0,
    )
    return taps, stride * slope


def sub_scan(total, sub):
    for step in (1, 2, 4):
        total = jnp.maximum(total, jnp.where(sub >= step, pltpu.roll(total, step, 0), NEG))
    return total


def kernel(
    nty, ntx, chunks, group, early,
    x_hbm, bearing_hbm, shift_hbm, camera_hbm, out,
    bearing, shift, camera, xs, top, bot, ls, wv, flat, scan,
    bpeaks, msg_i, msg_b, in_i, in_b, bsplat_i, bsplat_b, held,
    in_sem, tab_sem, ready, halo_send, halo_recv,
    pre_send_i, pre_recv_i, pre_send_b, pre_recv_b,
):
    ty = lax.axis_index("ty")
    tx = lax.axis_index("tx")
    width = chunks * LANES
    span = width * ntx
    tiles = ROWS // 8
    has_up = ty > 0
    has_down = ty < nty - 1
    mesh_id = pl.DeviceIdType.MESH

    in_i[...] = jnp.full(in_i.shape, NEG, jnp.float32)
    in_b[...] = jnp.full(in_b.shape, NEG, jnp.float32)

    barrier = pltpu.get_barrier_semaphore()

    def greet(p):
        pl.semaphore_signal(barrier, inc=1, device_id=p, device_id_type=mesh_id)

    @pl.when(has_up)
    def _():
        greet({"ty": ty - 1, "tx": tx})

    @pl.when(has_down)
    def _():
        greet({"ty": ty + 1, "tx": tx})

    for p in range(1, ntx):
        @pl.when(p > tx)
        def _():
            greet({"ty": ty, "tx": p})

    loads = [
        pltpu.make_async_copy(
            x_hbm.at[:, pl.ds(c * LANES, LANES)], xs.at[c], in_sem.at[c]
        )
        for c in range(chunks)
    ]
    small = [
        pltpu.make_async_copy(src, dst, tab_sem.at[n])
        for n, (src, dst) in enumerate(
            ((bearing_hbm, bearing), (shift_hbm, shift), (camera_hbm, camera))
        )
    ]
    for copy in small + loads:
        copy.start()
    for copy in small:
        copy.wait()

    for k in range(VIEWS):
        taps, rise = tables(bearing, camera, k, span)
        for j in range(4):
            wv[k, j] = taps[j]
        wv[k, 4] = rise

    for copy in loads:
        copy.wait()

    lane = lax.broadcasted_iota(jnp.int32, (8, LANES), 1)
    sub = lax.broadcasted_iota(jnp.int32, (8, LANES), 0)
    first = tx * width

    def ramp(k, c):
        return wv[k, 4] * (lane + (first + c * LANES)).astype(jnp.float32)

    def lift(src, c, k, start, slant):
        acc = wv[k, 0] * src[c, pl.ds(start - 1, 8), :]
        for j in range(1, 4):
            acc = acc + wv[k, j] * src[c, pl.ds(start + j - 1, 8), :]
        return acc + slant

    blank = jnp.zeros((8, LANES), jnp.float32)

    def block(c, k, n, carry):
        cols = pl.ds(pl.multiple_of(c * LANES, LANES), LANES)
        slant = ramp(k, c)
        parts = [blank]
        for i in range(1, tiles - 1):
            part = lift(xs, c, k, 8 * i + shift[k], slant)
            ls[k, 8 * i:8 * i + 8, cols] = part
            parts.append(part)
        parts.append(blank)
        turned = jnp.concatenate(parts, axis=0).T
        for t in range(16):
            at = 8 * t + t // 2
            flat[n, at:at + 8, :] = turned[8 * t:8 * t + 8]
        runs = [flat[n, pl.ds(0, 8, stride=17), :]]
        for u in range(1, 16):
            runs.append(jnp.maximum(runs[-1], flat[n, pl.ds(u, 8, stride=17), :]))
        total = sub_scan(runs[-1], sub)
        before = jnp.maximum(jnp.where(sub >= 1, pltpu.roll(total, 1, 0), NEG), carry)
        carry = jnp.maximum(carry, jnp.broadcast_to(total[7:8], (8, LANES)))
        for u in range(16):
            scan[n, pl.ds(u, 8, stride=17), :] = jnp.maximum(runs[u], before)
        whole = jnp.concatenate(
            [scan[n, 8 * t + t // 2:8 * t + t // 2 + 8, :] for t in range(16)], axis=0
        ).T
        for i in range(1, tiles - 1):
            out[k, 8 * i:8 * i + 8, cols] = whole[8 * i:8 * i + 8]
        return carry

    def interior(g, carries):
        carries = list(carries)
        for q in range(group):
            for k in range(VIEWS):
                carries[k] = block(g * group + q, k, q * VIEWS + k, carries[k])
        return tuple(carries)

    carries = tuple(jnp.full((8, LANES), NEG, jnp.float32) for _ in range(VIEWS))
    carries = lax.fori_loop(0, early, interior, carries)

    for c in range(chunks):
        top[c, 8:24] = xs[c, 0:16]
        bot[c, 0:16] = xs[c, ROWS - 16:ROWS]

    @pl.when(jnp.logical_not(has_up))
    def _():
        for c in range(chunks):
            top[c, 0:8] = blank

    @pl.when(jnp.logical_not(has_down))
    def _():
        for c in range(chunks):
            bot[c, 16:24] = blank

    pl.semaphore_wait(barrier, tx + has_up.astype(jnp.int32) + has_down.astype(jnp.int32))

    def halo(n, src_row, dst, dst_row, peer):
        return pltpu.make_async_remote_copy(
            src_ref=xs.at[:, pl.ds(src_row, 8), :], dst_ref=dst.at[:, pl.ds(dst_row, 8), :],
            send_sem=halo_send.at[n], recv_sem=halo_recv.at[n],
            device_id={"ty": peer, "tx": tx}, device_id_type=mesh_id,
        )

    @pl.when(has_up)
    def _():
        halo(0, 0, bot, 16, ty - 1).start()

    @pl.when(has_down)
    def _():
        halo(1, ROWS - 8, top, 0, ty + 1).start()

    for p in range(ntx - 1):
        @pl.when(p < tx)
        def _():
            pl.semaphore_signal(
                ready, inc=1, device_id={"ty": ty, "tx": p}, device_id_type=mesh_id
            )

    carries = lax.fori_loop(early, chunks // group, interior, carries)
    for k in range(VIEWS):
        msg_i[k] = carries[k][0:1]

    @pl.when(tx < ntx - 1)
    def _():
        pl.semaphore_wait(ready, ntx - 1 - tx)

    def message(msg, store, send, recv, p):
        return pltpu.make_async_remote_copy(
            src_ref=msg, dst_ref=store.at[tx], send_sem=send.at[p], recv_sem=recv.at[tx],
            device_id={"ty": ty, "tx": p}, device_id_type=mesh_id,
        )

    def spread(msg, store, send, recv):
        for p in range(1, ntx):
            @pl.when(p > tx)
            def _():
                message(msg, store, send, recv, p).start()

    def finish_sends(msg, store, send, recv):
        for p in range(1, ntx):
            @pl.when(p > tx)
            def _():
                message(msg, store, send, recv, p).wait_send()

    def receive(msg, store, recv):
        for p in range(ntx - 1):
            @pl.when(p < tx)
            def _():
                pltpu.make_async_remote_copy(
                    src_ref=msg, dst_ref=store.at[p], send_sem=recv.at[p], recv_sem=recv.at[p],
                    device_id={"ty": ty, "tx": p}, device_id_type=mesh_id,
                ).wait_recv()

    spread(msg_i, in_i, pre_send_i, pre_recv_i)

    @pl.when(has_down)
    def _():
        halo(0, 0, bot, 16, ty + 1).wait_recv()

    @pl.when(has_up)
    def _():
        halo(1, ROWS - 8, top, 0, ty - 1).wait_recv()

    edges = ((top, 0), (bot, ROWS - 8))
    bpeaks[...] = jnp.full(bpeaks.shape, NEG, jnp.float32)
    for k in range(VIEWS):
        for e, (src, row) in enumerate(edges):
            peak = None
            for c in range(chunks):
                part = lift(src, c, k, 8 + shift[k], ramp(k, c))
                ls[k, row:row + 8, c * LANES:(c + 1) * LANES] = part
                peak = part if peak is None else jnp.maximum(peak, part)
            bpeaks[16 * k + 8 * e:16 * k + 8 * e + 8, :] = peak
    msg_b[...] = jnp.max(bpeaks[...].T, axis=0, keepdims=True)
    spread(msg_b, in_b, pre_send_b, pre_recv_b)

    held[...] = jnp.full(held.shape, NEG, jnp.float32)

    def edge_scan(c, _):
        cols = pl.ds(pl.multiple_of(c * LANES, LANES), LANES)
        for k in range(VIEWS):
            for e, (_, row) in enumerate(edges):
                run = ls[k, row:row + 8, cols]
                step = 1
                while step < LANES:
                    run = jnp.maximum(
                        run, jnp.where(lane >= step, pltpu.roll(run, step, 1), NEG)
                    )
                    step *= 2
                run = jnp.maximum(run, held[2 * k + e])
                out[k, row:row + 8, cols] = run
                held[2 * k + e] = jnp.broadcast_to(run[:, LANES - 1:LANES], (8, LANES))
        return 0

    lax.fori_loop(0, chunks, edge_scan, 0)

    receive(msg_i, in_i, pre_recv_i)
    for k in range(VIEWS):
        best = in_i[0, k]
        for p in range(1, ntx):
            best = jnp.maximum(best, in_i[p, k])
        bsplat_i[k] = jnp.broadcast_to(best, (LANES, LANES)).T

    def close(k, row, before):
        for c in range(chunks):
            at = (k, pl.ds(row, 8), pl.ds(c * LANES, LANES))
            out[at] = jnp.maximum(out[at], before) - ls[at]

    def close_interior(i, _):
        row = pl.multiple_of(i * 8, 8)
        for k in range(VIEWS):
            close(k, row, bsplat_i[k, pl.ds(row, 8), :])
        return 0

    lax.fori_loop(1, tiles - 1, close_interior, 0)

    receive(msg_b, in_b, pre_recv_b)
    best = in_b[0]
    for p in range(1, ntx):
        best = jnp.maximum(best, in_b[p])
    bsplat_b[...] = jnp.broadcast_to(best, (LANES, LANES)).T
    for k in range(VIEWS):
        for e, (_, row) in enumerate(edges):
            close(k, row, bsplat_b[16 * k + 8 * e:16 * k + 8 * e + 8, :])

    @pl.when(has_up)
    def _():
        halo(0, 0, bot, 16, ty - 1).wait_send()

    @pl.when(has_down)
    def _():
        halo(1, ROWS - 8, top, 0, ty + 1).wait_send()

    finish_sends(msg_i, in_i, pre_send_i, pre_recv_i)
    finish_sends(msg_b, in_b, pre_send_b, pre_recv_b)


def on_device(surface_levels, bearing_index, stencil_displacements, camera_altitude_class):
    rows, width = surface_levels.shape
    nty, ntx = lax.axis_size("ty"), lax.axis_size("tx")
    chunks = width // LANES
    group, early = 2, 3
    vm = lambda *s: pltpu.VMEM(s, jnp.float32)
    arrays = [
        pltpu.with_memory_space_constraint(a, pltpu.HBM)
        for a in (surface_levels, bearing_index, stencil_displacements, camera_altitude_class)
    ]
    return pl.pallas_call(
        functools.partial(kernel, nty, ntx, chunks, group, early),
        out_shape=jax.ShapeDtypeStruct((VIEWS, rows, width), jnp.float32),
        in_specs=[pl.BlockSpec(memory_space=pltpu.HBM)] * 4,
        out_specs=pl.BlockSpec(memory_space=pltpu.VMEM),
        scratch_shapes=[
            pltpu.SMEM((VIEWS,), jnp.int32), pltpu.SMEM((VIEWS,), jnp.int32),
            pltpu.SMEM((VIEWS,), jnp.int32),
            vm(chunks, ROWS, LANES), vm(chunks, 24, LANES), vm(chunks, 24, LANES),
            vm(VIEWS, rows, width), vm(VIEWS, 5, 8, LANES),
            vm(group * VIEWS, 136, LANES), vm(group * VIEWS, 136, LANES),
            vm(LANES, LANES),
            vm(VIEWS, 1, LANES), vm(1, LANES),
            vm(ntx, VIEWS, 1, LANES), vm(ntx, 1, LANES),
            vm(VIEWS, LANES, LANES), vm(LANES, LANES), vm(2 * VIEWS, 8, LANES),
            pltpu.SemaphoreType.DMA((chunks,)),
            pltpu.SemaphoreType.DMA((3,)),
            pltpu.SemaphoreType.REGULAR,
            pltpu.SemaphoreType.DMA((2,)), pltpu.SemaphoreType.DMA((2,)),
            pltpu.SemaphoreType.DMA((ntx,)), pltpu.SemaphoreType.DMA((ntx,)),
            pltpu.SemaphoreType.DMA((ntx,)), pltpu.SemaphoreType.DMA((ntx,)),
        ],
        compiler_params=pltpu.CompilerParams(
            collective_id=0, has_side_effects=True, vmem_limit_bytes=40 * 1024 * 1024
        ),
        name="horizon",
    )(*arrays)


def solution(mesh):
    return jax.shard_map(
        on_device,
        mesh=mesh,
        in_specs=(P("ty", "tx"), P(), P(), P()),
        out_specs=P(None, "ty", "tx"),
        check_vma=False,
    )
```

```python
import functools
import math

import jax
import jax.numpy as jnp
from jax import lax
from jax.experimental import pallas as pl
from jax.experimental.pallas import tpu as pltpu
from jax.sharding import PartitionSpec as P

VIEWS = 4
ROWS = 128
LANES = 128
NEG = -jnp.inf


def tables(bearing, camera, k, span):
    a = jnp.full((8, LANES), bearing[k], jnp.int32)
    cls = jnp.full((8, LANES), camera[k], jnp.int32).astype(jnp.float32)
    f = (((a * 5) & 15).astype(jnp.float32) + 0.5) / 16.0
    theta = (a.astype(jnp.float32) - 7.5) * (math.pi / 32.0)
    stride = 1.0 / jnp.cos(theta)
    slope = (1.0 + cls) / (4.0 * span)
    cube = f * f * f
    square = f * f
    taps = (
        (-cube + 2.0 * square - f) / 2.0,
        (3.0 * cube - 5.0 * square + 2.0) / 2.0,
        (-3.0 * cube + 4.0 * square + f) / 2.0,
        (cube - square) / 2.0,
    )
    return taps, stride * slope


def sub_scan(total, sub):
    for step in (1, 2, 4):
        total = jnp.maximum(total, jnp.where(sub >= step, pltpu.roll(total, step, 0), NEG))
    return total


def kernel(
    nty, ntx, chunks, group, lead, near, far,
    x_hbm, bearing_hbm, shift_hbm, camera_hbm, out,
    tab, xs, top, bot, ls, wv, slants, flat, scan,
    peaks, bpeaks, msg_i, msg_b, in_i, in_b, bsplat_i, bsplat_b,
    in_sem, top_sem, bot_sem, tab_sem, ready, halo_send, halo_recv,
    send_i, recv_i, send_b, recv_b,
):
    ty = lax.axis_index("ty")
    tx = lax.axis_index("tx")
    width = chunks * LANES
    span = width * ntx
    tiles = ROWS // 8
    half = chunks // 2
    has_up = ty > 0
    has_down = ty < nty - 1
    mesh_id = pl.DeviceIdType.MESH
    barrier = pltpu.get_barrier_semaphore()

    def greet(p):
        pl.semaphore_signal(barrier, inc=1, device_id=p, device_id_type=mesh_id)

    @pl.when(has_up)
    def _():
        greet({"ty": ty - 1, "tx": tx})

    @pl.when(has_down)
    def _():
        greet({"ty": ty + 1, "tx": tx})

    for p in range(1, ntx):
        @pl.when(p > tx)
        def _():
            greet({"ty": ty, "tx": p})

    for c in range(chunks):
        cols = pl.ds(c * LANES, LANES)
        pltpu.make_async_copy(
            x_hbm.at[pl.ds(0, 16), cols], top.at[c, pl.ds(8, 16)], top_sem
        ).start()
        pltpu.make_async_copy(
            x_hbm.at[pl.ds(ROWS - 16, 16), cols], bot.at[c, pl.ds(0, 16)], bot_sem
        ).start()
    small = [
        pltpu.make_async_copy(src, tab.at[n], tab_sem.at[n])
        for n, src in enumerate((bearing_hbm, shift_hbm, camera_hbm))
    ]
    for copy in small:
        copy.start()
    for c in range(chunks):
        pltpu.make_async_copy(
            x_hbm.at[:, pl.ds(c * LANES, LANES)], xs.at[c], in_sem
        ).start()

    in_i[...] = jnp.full(in_i.shape, NEG, jnp.float32)
    in_b[...] = jnp.full(in_b.shape, NEG, jnp.float32)
    blank = jnp.zeros((8, LANES), jnp.float32)
    lowest = jnp.full((8, LANES), NEG, jnp.float32)

    @pl.when(jnp.logical_not(has_up))
    def _():
        for c in range(chunks):
            top[c, 0:8] = blank

    @pl.when(jnp.logical_not(has_down))
    def _():
        for c in range(chunks):
            bot[c, 16:24] = blank

    def arrived(rows, cols, sem):
        pltpu.make_async_copy(
            x_hbm.at[pl.ds(0, rows), pl.ds(0, cols)],
            ls.at[0, pl.ds(0, rows), pl.ds(0, cols)], sem,
        ).wait()

    arrived(16, width, top_sem)
    arrived(16, width, bot_sem)

    pl.semaphore_wait(barrier, tx + has_up.astype(jnp.int32) + has_down.astype(jnp.int32))

    def halo(n, peer):
        if n == 0:
            src, dst = top.at[:, pl.ds(8, 6), :], bot.at[:, pl.ds(16, 6), :]
        else:
            src, dst = bot.at[:, pl.ds(11, 5), :], top.at[:, pl.ds(3, 5), :]
        return pltpu.make_async_remote_copy(
            src_ref=src, dst_ref=dst, send_sem=halo_send.at[n], recv_sem=halo_recv.at[n],
            device_id={"ty": peer, "tx": tx}, device_id_type=mesh_id,
        )

    @pl.when(has_up)
    def _():
        halo(0, ty - 1).start()

    @pl.when(has_down)
    def _():
        halo(1, ty + 1).start()

    for p in range(ntx - 1):
        @pl.when(p < tx)
        def _():
            pl.semaphore_signal(
                ready, inc=1, device_id={"ty": ty, "tx": p}, device_id_type=mesh_id
            )

    for copy in small:
        copy.wait()
    bearing, shift, camera = (
        [tab[n, k] for k in range(VIEWS)] for n in range(3)
    )
    lane = lax.broadcasted_iota(jnp.int32, (8, LANES), 1)
    sub = lax.broadcasted_iota(jnp.int32, (8, LANES), 0)
    first = tx * width
    for k in range(VIEWS):
        taps, rise = tables(bearing, camera, k, span)
        for j in range(4):
            wv[k, j] = taps[j]
        for c in range(chunks):
            slants[k, c] = rise * (lane + (first + c * LANES)).astype(jnp.float32)

    for k in range(VIEWS):
        peaks[k, 0:8, :] = lowest
        peaks[k, ROWS - 8:ROWS, :] = lowest

    arrived(ROWS, width, in_sem)

    def lift(src, c, k, start):
        acc = wv[k, 0] * src[c, pl.ds(start - 1, 8), :]
        for j in range(1, 4):
            acc = acc + wv[k, j] * src[c, pl.ds(start + j - 1, 8), :]
        return acc + slants[k, c]

    def lift_interior(i, _):
        row = pl.multiple_of(i * 8, 8)
        for k in range(VIEWS):
            peak = None
            for c in range(chunks):
                part = lift(xs, c, k, row + shift[k])
                ls[k, pl.ds(row, 8), c * LANES:(c + 1) * LANES] = part
                peak = part if peak is None else jnp.maximum(peak, part)
            peaks[k, pl.ds(row, 8), :] = peak
        return 0

    lax.fori_loop(1, tiles - 1, lift_interior, 0)
    for k in range(VIEWS):
        msg_i[k] = jnp.max(peaks[k].T, axis=0, keepdims=True)

    def spread(msg, store, send, recv):
        for p in range(ntx - 1, 0, -1):
            @pl.when(p > tx)
            def _():
                pltpu.make_async_remote_copy(
                    src_ref=msg, dst_ref=store.at[tx], send_sem=send, recv_sem=recv,
                    device_id={"ty": ty, "tx": p}, device_id_type=mesh_id,
                ).start()

    def all_of(store, send, recv, n):
        some = store.at[pl.ds(0, n)]
        return pltpu.make_async_remote_copy(
            src_ref=some, dst_ref=some, send_sem=send, recv_sem=recv,
            device_id={"ty": ty, "tx": tx}, device_id_type=mesh_id,
        )

    def finish_sends(store, send, recv):
        for n in range(1, ntx):
            @pl.when(ntx - 1 - tx == n)
            def _():
                all_of(store, send, recv, n).wait_send()

    def receive(store, send, recv):
        for n in range(1, ntx):
            @pl.when(tx == n)
            def _():
                all_of(store, send, recv, n).wait_recv()

    def turn_scan(parts, n, carry):
        turned = jnp.concatenate(parts, axis=0).T
        for t in range(16):
            at = 8 * t + t // 2
            flat[n, at:at + 8, :] = turned[8 * t:8 * t + 8]
        runs = [flat[n, pl.ds(0, 8, stride=17), :]]
        for u in range(1, 16):
            runs.append(jnp.maximum(runs[-1], flat[n, pl.ds(u, 8, stride=17), :]))
        total = sub_scan(runs[-1], sub)
        before = jnp.maximum(jnp.where(sub >= 1, pltpu.roll(total, 1, 0), NEG), carry)
        carry = jnp.maximum(carry, jnp.broadcast_to(total[7:8], (8, LANES)))
        for u in range(16):
            scan[n, pl.ds(u, 8, stride=17), :] = jnp.maximum(runs[u], before)
        whole = jnp.concatenate(
            [scan[n, 8 * t + t // 2:8 * t + t // 2 + 8, :] for t in range(16)], axis=0
        ).T
        return whole, carry

    def interior(g, carries):
        carries = list(carries)
        for q in range(group):
            c = g * group + q
            cols = pl.ds(pl.multiple_of(c * LANES, LANES), LANES)
            for k in range(VIEWS):
                parts = [blank] + [
                    ls[k, 8 * i:8 * i + 8, cols] for i in range(1, tiles - 1)
                ] + [blank]
                whole, carries[k] = turn_scan(parts, q * VIEWS + k, carries[k])
                for i in range(1, tiles - 1):
                    out[k, 8 * i:8 * i + 8, cols] = whole[8 * i:8 * i + 8]
        return tuple(carries)

    middle = jnp.logical_or(ty == nty // 2, ty == nty // 2 - 1)
    ahead = jnp.where(middle, far, near)
    carries = lax.fori_loop(0, lead, interior, (lowest,) * VIEWS)

    @pl.when(tx < ntx - 1)
    def _():
        pl.semaphore_wait(ready, ntx - 1 - tx)

    spread(msg_i, in_i, send_i, recv_i)
    carries = lax.fori_loop(lead, ahead, interior, carries)

    @pl.when(has_down)
    def _():
        halo(0, ty + 1).wait_recv()

    @pl.when(has_up)
    def _():
        halo(1, ty - 1).wait_recv()

    edges = ((top, 0), (bot, ROWS - 8))
    for k in range(VIEWS):
        for e, (src, row) in enumerate(edges):
            at = 16 * k + 8 * e
            halves = []
            for h in range(2):
                peak = None
                for c in range(h * half, (h + 1) * half):
                    part = lift(src, c, k, 8 + shift[k])
                    ls[k, row:row + 8, c * LANES:(c + 1) * LANES] = part
                    peak = part if peak is None else jnp.maximum(peak, part)
                halves.append(peak)
            bpeaks[at:at + 8, :] = jnp.maximum(halves[0], halves[1])
            bpeaks[64 + at:72 + at, :] = halves[0]
    msg_b[...] = jnp.max(bpeaks[...].T, axis=0, keepdims=True)
    spread(msg_b, in_b, send_b, recv_b)

    lax.fori_loop(ahead, chunks // group, interior, carries)

    carry = lowest
    for c in range(half):
        places = [
            (k, row, pl.ds((c + h * half) * LANES, LANES))
            for h in range(2) for k in range(VIEWS) for _, row in edges
        ]
        parts = [ls[k, row:row + 8, cols] for k, row, cols in places]
        whole, carry = turn_scan(parts, c, carry)
        for n, (k, row, cols) in enumerate(places):
            out[k, row:row + 8, cols] = whole[8 * n:8 * n + 8]

    receive(in_i, send_i, recv_i)
    for k in range(VIEWS):
        best = in_i[0, k]
        for p in range(1, ntx):
            best = jnp.maximum(best, in_i[p, k])
        bsplat_i[k] = jnp.broadcast_to(best, (LANES, LANES)).T

    def close(k, row, before, span):
        for c in span:
            at = (k, pl.ds(row, 8), pl.ds(c * LANES, LANES))
            out[at] = jnp.maximum(out[at], before) - ls[at]

    def close_interior(i, _):
        row = pl.multiple_of(i * 8, 8)
        for k in range(VIEWS):
            close(k, row, bsplat_i[k, pl.ds(row, 8), :], range(chunks))
        return 0

    lax.fori_loop(1, tiles - 1, close_interior, 0)

    @pl.when(has_up)
    def _():
        halo(0, ty - 1).wait_send()

    @pl.when(has_down)
    def _():
        halo(1, ty + 1).wait_send()

    finish_sends(in_i, send_i, recv_i)
    finish_sends(in_b, send_b, recv_b)

    receive(in_b, send_b, recv_b)
    best = in_b[0]
    for p in range(1, ntx):
        best = jnp.maximum(best, in_b[p])
    bsplat_b[...] = jnp.broadcast_to(best, (LANES, LANES)).T
    for k in range(VIEWS):
        for e, (_, row) in enumerate(edges):
            at = 16 * k + 8 * e
            before = bsplat_b[at:at + 8, :]
            close(k, row, before, range(half))
            own = jnp.max(bpeaks[64 + at:72 + at, :], axis=1, keepdims=True)
            close(k, row, jnp.maximum(before, own), range(half, chunks))


def on_device(surface_levels, bearing_index, stencil_displacements, camera_altitude_class):
    rows, width = surface_levels.shape
    nty, ntx = lax.axis_size("ty"), lax.axis_size("tx")
    chunks = width // LANES
    group, lead, near, far = 4, 0, 0, 1
    vm = lambda *s: pltpu.VMEM(s, jnp.float32)
    dma = pltpu.SemaphoreType.DMA
    arrays = [
        pltpu.with_memory_space_constraint(a, pltpu.HBM)
        for a in (surface_levels, bearing_index, stencil_displacements, camera_altitude_class)
    ]
    return pl.pallas_call(
        functools.partial(kernel, nty, ntx, chunks, group, lead, near, far),
        out_shape=jax.ShapeDtypeStruct((VIEWS, rows, width), jnp.float32),
        in_specs=[pl.BlockSpec(memory_space=pltpu.HBM)] * 4,
        out_specs=pl.BlockSpec(memory_space=pltpu.VMEM),
        scratch_shapes=[
            pltpu.SMEM((3, VIEWS), jnp.int32),
            vm(chunks, ROWS, LANES), vm(chunks, 24, LANES), vm(chunks, 24, LANES),
            vm(VIEWS, rows, width), vm(VIEWS, 4, 8, LANES), vm(VIEWS, chunks, 8, LANES),
            vm(group * VIEWS, 136, LANES), vm(group * VIEWS, 136, LANES),
            vm(VIEWS, ROWS, LANES), vm(LANES, LANES),
            vm(VIEWS, 1, LANES), vm(1, LANES),
            vm(ntx, VIEWS, 1, LANES), vm(ntx, 1, LANES),
            vm(VIEWS, LANES, LANES), vm(LANES, LANES),
            dma, dma, dma, dma((3,)),
            pltpu.SemaphoreType.REGULAR,
            dma((2,)), dma((2,)), dma, dma, dma, dma,
        ],
        compiler_params=pltpu.CompilerParams(
            collective_id=0, has_side_effects=True, vmem_limit_bytes=40 * 1024 * 1024
        ),
        name="horizon",
    )(*arrays)


def solution(mesh):
    return jax.shard_map(
        on_device,
        mesh=mesh,
        in_specs=(P("ty", "tx"), P(), P(), P()),
        out_specs=P(None, "ty", "tx"),
        check_vma=False,
    )
```

```python
import functools
import math

import jax
import jax.numpy as jnp
from jax import lax
from jax.experimental import pallas as pl
from jax.experimental.pallas import tpu as pltpu
from jax.sharding import PartitionSpec as P

VIEWS = 4
ROWS = 128
LANES = 128
NEG = -jnp.inf


def tables(bearing, camera, k, span):
    a = jnp.full((8, LANES), bearing[k], jnp.int32)
    cls = jnp.full((8, LANES), camera[k], jnp.int32).astype(jnp.float32)
    f = (((a * 5) & 15).astype(jnp.float32) + 0.5) / 16.0
    theta = (a.astype(jnp.float32) - 7.5) * (math.pi / 32.0)
    stride = 1.0 / jnp.cos(theta)
    slope = (1.0 + cls) / (4.0 * span)
    cube = f * f * f
    square = f * f
    taps = (
        (-cube + 2.0 * square - f) / 2.0,
        (3.0 * cube - 5.0 * square + 2.0) / 2.0,
        (-3.0 * cube + 4.0 * square + f) / 2.0,
        (cube - square) / 2.0,
    )
    return taps, stride * slope


def sub_scan(total, sub):
    for step in (1, 2, 4):
        total = jnp.maximum(total, jnp.where(sub >= step, pltpu.roll(total, step, 0), NEG))
    return total


def kernel(
    nty, ntx, chunks, group, pre, near, far,
    x_hbm, bearing_hbm, shift_hbm, camera_hbm, out,
    tab, xs, top0, top1, bot0, bot1, ls, wv, slants, flat, scan,
    peaks, bpeaks, msg_i, msg_b, in_i, in_b, bsplat_i, bsplat_b,
    in_sem, top_sem, bot_sem, tab_sem, halo_send, halo_recv,
    send_i, recv_i, send_b, recv_b,
):
    ty = lax.axis_index("ty")
    tx = lax.axis_index("tx")
    width = chunks * LANES
    span = width * ntx
    tiles = ROWS // 8
    half = chunks // 2
    has_up = ty > 0
    has_down = ty < nty - 1
    mesh_id = pl.DeviceIdType.MESH
    barrier = pltpu.get_barrier_semaphore()
    top, bot = (top0, top1), (bot0, bot1)

    def greet(p):
        pl.semaphore_signal(barrier, inc=1, device_id=p, device_id_type=mesh_id)

    @pl.when(has_up)
    def _():
        greet({"ty": ty - 1, "tx": tx})

    @pl.when(has_down)
    def _():
        greet({"ty": ty + 1, "tx": tx})

    for p in range(ntx - 1):
        @pl.when(p < tx)
        def _():
            greet({"ty": ty, "tx": p})

    for c in range(chunks):
        cols = pl.ds(c * LANES, LANES)
        pltpu.make_async_copy(
            x_hbm.at[pl.ds(0, 16), cols], top[c // half].at[c % half, pl.ds(8, 16)], top_sem
        ).start()
        pltpu.make_async_copy(
            x_hbm.at[pl.ds(ROWS - 16, 16), cols], bot[c // half].at[c % half, pl.ds(0, 16)],
            bot_sem,
        ).start()
    small = [
        pltpu.make_async_copy(src, tab.at[n], tab_sem.at[n])
        for n, src in enumerate((bearing_hbm, shift_hbm, camera_hbm))
    ]
    for copy in small:
        copy.start()
    for c in range(chunks):
        pltpu.make_async_copy(
            x_hbm.at[:, pl.ds(c * LANES, LANES)], xs.at[c], in_sem
        ).start()

    blank = jnp.zeros((8, LANES), jnp.float32)
    lowest = jnp.full((8, LANES), NEG, jnp.float32)

    @pl.when(jnp.logical_not(has_up))
    def _():
        for c in range(chunks):
            top[c // half][c % half, 0:8] = blank

    @pl.when(jnp.logical_not(has_down))
    def _():
        for c in range(chunks):
            bot[c // half][c % half, 16:24] = blank

    def arrived(rows, cols, sem):
        pltpu.make_async_copy(
            x_hbm.at[pl.ds(0, rows), pl.ds(0, cols)],
            ls.at[0, pl.ds(0, rows), pl.ds(0, cols)], sem,
        ).wait()

    arrived(16, width, top_sem)
    arrived(16, width, bot_sem)

    for copy in small:
        copy.wait()
    bearing, shift, camera = (
        [tab[n, k] for k in range(VIEWS)] for n in range(3)
    )
    lane = lax.broadcasted_iota(jnp.int32, (8, LANES), 1)
    sub = lax.broadcasted_iota(jnp.int32, (8, LANES), 0)
    first = tx * width
    for k in range(VIEWS):
        taps, rise = tables(bearing, camera, k, span)
        for j in range(4):
            wv[k, j] = taps[j]
        for c in range(chunks):
            slants[k, c] = rise * (lane + (first + c * LANES)).astype(jnp.float32)

    for k in range(VIEWS):
        peaks[k, 0:8, :] = lowest
        peaks[k, ROWS - 8:ROWS, :] = lowest

    arrived(ROWS, width, in_sem)

    def lift(src, at, c, k, start):
        acc = wv[k, 0] * src[at, pl.ds(start - 1, 8), :]
        for j in range(1, 4):
            acc = acc + wv[k, j] * src[at, pl.ds(start + j - 1, 8), :]
        return acc + slants[k, c]

    def lift_interior(i, _):
        row = pl.multiple_of(i * 8, 8)
        for k in range(VIEWS):
            peak = None
            for c in range(chunks):
                part = lift(xs, c, c, k, row + shift[k])
                ls[k, pl.ds(row, 8), c * LANES:(c + 1) * LANES] = part
                peak = part if peak is None else jnp.maximum(peak, part)
            peaks[k, pl.ds(row, 8), :] = peak
        return 0

    lax.fori_loop(1, 1 + pre, lift_interior, 0)

    pl.semaphore_wait(
        barrier, (ntx - 1 - tx) + has_up.astype(jnp.int32) + has_down.astype(jnp.int32)
    )

    def halo(n, h, peer):
        if n == 0:
            src, dst = top[h].at[:, pl.ds(8, 6), :], bot[h].at[:, pl.ds(16, 6), :]
        else:
            src, dst = bot[h].at[:, pl.ds(11, 5), :], top[h].at[:, pl.ds(3, 5), :]
        return pltpu.make_async_remote_copy(
            src_ref=src, dst_ref=dst,
            send_sem=halo_send.at[n, h], recv_sem=halo_recv.at[n, h],
            device_id={"ty": peer, "tx": tx}, device_id_type=mesh_id,
        )

    @pl.when(has_up)
    def _():
        for h in range(2):
            halo(0, h, ty - 1).start()

    @pl.when(has_down)
    def _():
        for h in range(2):
            halo(1, h, ty + 1).start()

    lax.fori_loop(1 + pre, tiles - 1, lift_interior, 0)
    for k in range(VIEWS):
        msg_i[k] = jnp.max(peaks[k].T, axis=0, keepdims=True)

    def spread(msg, store, send, recv):
        for p in range(ntx - 1, 0, -1):
            @pl.when(p > tx)
            def _():
                pltpu.make_async_remote_copy(
                    src_ref=msg, dst_ref=store.at[tx], send_sem=send, recv_sem=recv,
                    device_id={"ty": ty, "tx": p}, device_id_type=mesh_id,
                ).start()

    def all_of(store, send, recv, n):
        some = store.at[pl.ds(0, n)]
        return pltpu.make_async_remote_copy(
            src_ref=some, dst_ref=some, send_sem=send, recv_sem=recv,
            device_id={"ty": ty, "tx": tx}, device_id_type=mesh_id,
        )

    def finish_sends(store, send, recv):
        for n in range(1, ntx):
            @pl.when(ntx - 1 - tx == n)
            def _():
                all_of(store, send, recv, n).wait_send()

    def receive(store, send, recv):
        for n in range(1, ntx):
            @pl.when(tx == n)
            def _():
                all_of(store, send, recv, n).wait_recv()

    def turn_scan(parts, n, carry):
        turned = jnp.concatenate(parts, axis=0).T
        for t in range(16):
            at = 8 * t + t // 2
            flat[n, at:at + 8, :] = turned[8 * t:8 * t + 8]
        runs = [flat[n, pl.ds(0, 8, stride=17), :]]
        for u in range(1, 16):
            runs.append(jnp.maximum(runs[-1], flat[n, pl.ds(u, 8, stride=17), :]))
        total = sub_scan(runs[-1], sub)
        before = jnp.maximum(jnp.where(sub >= 1, pltpu.roll(total, 1, 0), NEG), carry)
        carry = jnp.maximum(carry, jnp.broadcast_to(total[7:8], (8, LANES)))
        for u in range(16):
            scan[n, pl.ds(u, 8, stride=17), :] = jnp.maximum(runs[u], before)
        whole = jnp.concatenate(
            [scan[n, 8 * t + t // 2:8 * t + t // 2 + 8, :] for t in range(16)], axis=0
        ).T
        return whole, carry

    def interior(g, carries):
        carries = list(carries)
        for q in range(group):
            c = g * group + q
            cols = pl.ds(pl.multiple_of(c * LANES, LANES), LANES)
            for k in range(VIEWS):
                parts = [blank] + [
                    ls[k, 8 * i:8 * i + 8, cols] for i in range(1, tiles - 1)
                ] + [blank]
                whole, carries[k] = turn_scan(parts, q * VIEWS + k, carries[k])
                for i in range(1, tiles - 1):
                    out[k, 8 * i:8 * i + 8, cols] = whole[8 * i:8 * i + 8]
        return tuple(carries)

    middle = jnp.logical_or(ty == nty // 2, ty == nty // 2 - 1)
    ahead = jnp.where(middle, far, near)
    spread(msg_i, in_i, send_i, recv_i)
    carries = lax.fori_loop(0, ahead, interior, (lowest,) * VIEWS)

    edges = ((top, 0), (bot, ROWS - 8))
    for h in range(2):
        @pl.when(has_down)
        def _():
            halo(0, h, ty + 1).wait_recv()

        @pl.when(has_up)
        def _():
            halo(1, h, ty - 1).wait_recv()

        for k in range(VIEWS):
            for e, (src, row) in enumerate(edges):
                at = 16 * k + 8 * e
                peak = None if h == 0 else bpeaks[64 + at:72 + at, :]
                for c in range(h * half, (h + 1) * half):
                    part = lift(src[h], c - h * half, c, k, 8 + shift[k])
                    ls[k, row:row + 8, c * LANES:(c + 1) * LANES] = part
                    peak = part if peak is None else jnp.maximum(peak, part)
                at = at + 64 if h == 0 else at
                bpeaks[at:at + 8, :] = peak
    msg_b[...] = jnp.max(bpeaks[...].T, axis=0, keepdims=True)
    spread(msg_b, in_b, send_b, recv_b)

    lax.fori_loop(ahead, chunks // group, interior, carries)

    carry = lowest
    for c in range(half):
        places = [
            (k, row, pl.ds((c + h * half) * LANES, LANES))
            for h in range(2) for k in range(VIEWS) for _, row in edges
        ]
        parts = [ls[k, row:row + 8, cols] for k, row, cols in places]
        whole, carry = turn_scan(parts, c, carry)
        for n, (k, row, cols) in enumerate(places):
            out[k, row:row + 8, cols] = whole[8 * n:8 * n + 8]

    receive(in_i, send_i, recv_i)
    for k in range(VIEWS):
        best = jnp.full((1, LANES), NEG, jnp.float32)
        for p in range(ntx - 1):
            best = jnp.maximum(best, jnp.where(p < tx, in_i[p, k], NEG))
        bsplat_i[k] = jnp.broadcast_to(best, (LANES, LANES)).T

    def close(k, row, before, span):
        for c in span:
            at = (k, pl.ds(row, 8), pl.ds(c * LANES, LANES))
            out[at] = jnp.maximum(out[at], before) - ls[at]

    def close_interior(i, _):
        row = pl.multiple_of(i * 8, 8)
        for k in range(VIEWS):
            close(k, row, bsplat_i[k, pl.ds(row, 8), :], range(chunks))
        return 0

    lax.fori_loop(1, tiles - 1, close_interior, 0)

    @pl.when(has_up)
    def _():
        for h in range(2):
            halo(0, h, ty - 1).wait_send()

    @pl.when(has_down)
    def _():
        for h in range(2):
            halo(1, h, ty + 1).wait_send()

    finish_sends(in_i, send_i, recv_i)
    finish_sends(in_b, send_b, recv_b)

    receive(in_b, send_b, recv_b)
    best = jnp.full((1, LANES), NEG, jnp.float32)
    for p in range(ntx - 1):
        best = jnp.maximum(best, jnp.where(p < tx, in_b[p], NEG))
    bsplat_b[...] = jnp.broadcast_to(best, (LANES, LANES)).T
    for k in range(VIEWS):
        for e, (_, row) in enumerate(edges):
            at = 16 * k + 8 * e
            before = bsplat_b[at:at + 8, :]
            close(k, row, before, range(half))
            own = jnp.max(bpeaks[64 + at:72 + at, :], axis=1, keepdims=True)
            close(k, row, jnp.maximum(before, own), range(half, chunks))


def on_device(surface_levels, bearing_index, stencil_displacements, camera_altitude_class):
    rows, width = surface_levels.shape
    nty, ntx = lax.axis_size("ty"), lax.axis_size("tx")
    chunks = width // LANES
    group, pre, near, far = 4, 5, 1, 3
    vm = lambda *s: pltpu.VMEM(s, jnp.float32)
    dma = pltpu.SemaphoreType.DMA
    arrays = [
        pltpu.with_memory_space_constraint(a, pltpu.HBM)
        for a in (surface_levels, bearing_index, stencil_displacements, camera_altitude_class)
    ]
    return pl.pallas_call(
        functools.partial(kernel, nty, ntx, chunks, group, pre, near, far),
        out_shape=jax.ShapeDtypeStruct((VIEWS, rows, width), jnp.float32),
        in_specs=[pl.BlockSpec(memory_space=pltpu.HBM)] * 4,
        out_specs=pl.BlockSpec(memory_space=pltpu.VMEM),
        scratch_shapes=[
            pltpu.SMEM((3, VIEWS), jnp.int32),
            vm(chunks, ROWS, LANES)] + [vm(chunks // 2, 24, LANES)] * 4 + [
            vm(VIEWS, rows, width), vm(VIEWS, 4, 8, LANES), vm(VIEWS, chunks, 8, LANES),
            vm(group * VIEWS, 136, LANES), vm(group * VIEWS, 136, LANES),
            vm(VIEWS, ROWS, LANES), vm(LANES, LANES),
            vm(VIEWS, 1, LANES), vm(1, LANES),
            vm(ntx, VIEWS, 1, LANES), vm(ntx, 1, LANES),
            vm(VIEWS, LANES, LANES), vm(LANES, LANES),
            dma, dma, dma, dma((3,)),
            dma((2, 2)), dma((2, 2)), dma, dma, dma, dma,
        ],
        compiler_params=pltpu.CompilerParams(
            collective_id=0, has_side_effects=True, vmem_limit_bytes=40 * 1024 * 1024
        ),
        name="horizon",
    )(*arrays)


def solution(mesh):
    return jax.shard_map(
        on_device,
        mesh=mesh,
        in_specs=(P("ty", "tx"), P(), P(), P()),
        out_specs=P(None, "ty", "tx"),
        check_vma=False,
    )
```

```python
import functools
import math

import jax
import jax.numpy as jnp
from jax import lax
from jax.experimental import pallas as pl
from jax.experimental.pallas import tpu as pltpu
from jax.sharding import PartitionSpec as P

VIEWS = 4
ROWS = 128
LANES = 128
NEG = -jnp.inf


def tables(bearing, camera, k, span):
    a = jnp.full((8, LANES), bearing[k], jnp.int32)
    cls = jnp.full((8, LANES), camera[k], jnp.int32).astype(jnp.float32)
    f = (((a * 5) & 15).astype(jnp.float32) + 0.5) / 16.0
    theta = (a.astype(jnp.float32) - 7.5) * (math.pi / 32.0)
    stride = 1.0 / jnp.cos(theta)
    slope = (1.0 + cls) / (4.0 * span)
    cube = f * f * f
    square = f * f
    taps = (
        (-cube + 2.0 * square - f) / 2.0,
        (3.0 * cube - 5.0 * square + 2.0) / 2.0,
        (-3.0 * cube + 4.0 * square + f) / 2.0,
        (cube - square) / 2.0,
    )
    return taps, stride * slope


def sub_scan(total, sub):
    for step in (1, 2, 4):
        total = jnp.maximum(total, jnp.where(sub >= step, pltpu.roll(total, step, 0), NEG))
    return total


def kernel(
    nty, ntx, chunks, group, pre, near, far,
    x_hbm, bearing_hbm, shift_hbm, camera_hbm, out, sums, before_b, firsts,
    tab, xs, top0, top1, bot0, bot1, ls, wv, slants, flat, scan,
    peaks, bpeaks, msg_i, msg_b, in_i, in_b, bsplat_i,
    in_sem, top_sem, bot_sem, tab_sem, halo_send, halo_recv,
    send_i, recv_i, send_b, recv_b,
):
    ty = lax.axis_index("ty")
    tx = lax.axis_index("tx")
    width = chunks * LANES
    span = width * ntx
    tiles = ROWS // 8
    half = chunks // 2
    has_up = ty > 0
    has_down = ty < nty - 1
    mesh_id = pl.DeviceIdType.MESH
    barrier = pltpu.get_barrier_semaphore()
    top, bot = (top0, top1), (bot0, bot1)

    def greet(p):
        pl.semaphore_signal(barrier, inc=1, device_id=p, device_id_type=mesh_id)

    @pl.when(has_up)
    def _():
        greet({"ty": ty - 1, "tx": tx})

    @pl.when(has_down)
    def _():
        greet({"ty": ty + 1, "tx": tx})

    for p in range(ntx - 1):
        @pl.when(p < tx)
        def _():
            greet({"ty": ty, "tx": p})

    for c in range(chunks):
        cols = pl.ds(c * LANES, LANES)
        pltpu.make_async_copy(
            x_hbm.at[pl.ds(0, 16), cols], top[c // half].at[c % half, pl.ds(8, 16)], top_sem
        ).start()
        pltpu.make_async_copy(
            x_hbm.at[pl.ds(ROWS - 16, 16), cols], bot[c // half].at[c % half, pl.ds(0, 16)],
            bot_sem,
        ).start()
    small = [
        pltpu.make_async_copy(src, tab.at[n], tab_sem.at[n])
        for n, src in enumerate((bearing_hbm, shift_hbm, camera_hbm))
    ]
    for copy in small:
        copy.start()
    for c in range(chunks):
        pltpu.make_async_copy(
            x_hbm.at[:, pl.ds(c * LANES, LANES)], xs.at[c], in_sem
        ).start()

    blank = jnp.zeros((8, LANES), jnp.float32)
    lowest = jnp.full((8, LANES), NEG, jnp.float32)

    @pl.when(jnp.logical_not(has_up))
    def _():
        for c in range(chunks):
            top[c // half][c % half, 0:8] = blank

    @pl.when(jnp.logical_not(has_down))
    def _():
        for c in range(chunks):
            bot[c // half][c % half, 16:24] = blank

    def arrived(rows, cols, sem):
        pltpu.make_async_copy(
            x_hbm.at[pl.ds(0, rows), pl.ds(0, cols)],
            ls.at[0, pl.ds(0, rows), pl.ds(0, cols)], sem,
        ).wait()

    arrived(16, width, top_sem)
    arrived(16, width, bot_sem)

    for copy in small:
        copy.wait()
    bearing, shift, camera = (
        [tab[n, k] for k in range(VIEWS)] for n in range(3)
    )
    lane = lax.broadcasted_iota(jnp.int32, (8, LANES), 1)
    sub = lax.broadcasted_iota(jnp.int32, (8, LANES), 0)
    first = tx * width
    for k in range(VIEWS):
        taps, rise = tables(bearing, camera, k, span)
        for j in range(4):
            wv[k, j] = taps[j]
        for c in range(chunks):
            slants[k, c] = rise * (lane + (first + c * LANES)).astype(jnp.float32)

    for k in range(VIEWS):
        peaks[k, 0:8, :] = lowest
        peaks[k, ROWS - 8:ROWS, :] = lowest

    arrived(ROWS, width, in_sem)

    def lift(src, at, c, k, start):
        acc = wv[k, 0] * src[at, pl.ds(start - 1, 8), :]
        for j in range(1, 4):
            acc = acc + wv[k, j] * src[at, pl.ds(start + j - 1, 8), :]
        return acc + slants[k, c]

    def lift_interior(i, _):
        row = pl.multiple_of(i * 8, 8)
        for k in range(VIEWS):
            peak = None
            for c in range(chunks):
                part = lift(xs, c, c, k, row + shift[k])
                ls[k, pl.ds(row, 8), c * LANES:(c + 1) * LANES] = part
                peak = part if peak is None else jnp.maximum(peak, part)
            peaks[k, pl.ds(row, 8), :] = peak
        return 0

    lax.fori_loop(1, 1 + pre, lift_interior, 0)

    pl.semaphore_wait(
        barrier, (ntx - 1 - tx) + has_up.astype(jnp.int32) + has_down.astype(jnp.int32)
    )

    def halo(n, h, peer):
        if n == 0:
            src, dst = top[h].at[:, pl.ds(8, 6), :], bot[h].at[:, pl.ds(16, 6), :]
        else:
            src, dst = bot[h].at[:, pl.ds(11, 5), :], top[h].at[:, pl.ds(3, 5), :]
        return pltpu.make_async_remote_copy(
            src_ref=src, dst_ref=dst,
            send_sem=halo_send.at[n, h], recv_sem=halo_recv.at[n, h],
            device_id={"ty": peer, "tx": tx}, device_id_type=mesh_id,
        )

    @pl.when(has_up)
    def _():
        for h in range(2):
            halo(0, h, ty - 1).start()

    @pl.when(has_down)
    def _():
        for h in range(2):
            halo(1, h, ty + 1).start()

    lax.fori_loop(1 + pre, tiles - 1, lift_interior, 0)
    for k in range(VIEWS):
        msg_i[k] = jnp.max(peaks[k].T, axis=0, keepdims=True)

    def spread(msg, store, send, recv):
        for p in list(range(ntx // 2, ntx)) + list(range(1, ntx // 2)):
            @pl.when(p > tx)
            def _():
                pltpu.make_async_remote_copy(
                    src_ref=msg, dst_ref=store.at[tx], send_sem=send, recv_sem=recv,
                    device_id={"ty": ty, "tx": p}, device_id_type=mesh_id,
                ).start()

    def all_of(store, send, recv, n):
        some = store.at[pl.ds(0, n)]
        return pltpu.make_async_remote_copy(
            src_ref=some, dst_ref=some, send_sem=send, recv_sem=recv,
            device_id={"ty": ty, "tx": tx}, device_id_type=mesh_id,
        )

    def finish_sends(store, send, recv):
        for n in range(1, ntx):
            @pl.when(ntx - 1 - tx == n)
            def _():
                all_of(store, send, recv, n).wait_send()

    def receive(store, send, recv):
        for n in range(1, ntx):
            @pl.when(tx == n)
            def _():
                all_of(store, send, recv, n).wait_recv()

    def turn_scan(parts, n, carry):
        turned = jnp.concatenate(parts, axis=0).T
        for t in range(16):
            at = 8 * t + t // 2
            flat[n, at:at + 8, :] = turned[8 * t:8 * t + 8]
        runs = [flat[n, pl.ds(0, 8, stride=17), :]]
        for u in range(1, 16):
            runs.append(jnp.maximum(runs[-1], flat[n, pl.ds(u, 8, stride=17), :]))
        total = sub_scan(runs[-1], sub)
        before = jnp.maximum(jnp.where(sub >= 1, pltpu.roll(total, 1, 0), NEG), carry)
        carry = jnp.maximum(carry, jnp.broadcast_to(total[7:8], (8, LANES)))
        for u in range(16):
            scan[n, pl.ds(u, 8, stride=17), :] = jnp.maximum(runs[u], before)
        whole = jnp.concatenate(
            [scan[n, 8 * t + t // 2:8 * t + t // 2 + 8, :] for t in range(16)], axis=0
        ).T
        return whole, carry

    def interior(g, carries):
        carries = list(carries)
        for q in range(group):
            c = g * group + q
            cols = pl.ds(pl.multiple_of(c * LANES, LANES), LANES)
            for k in range(VIEWS):
                parts = [blank] + [
                    ls[k, 8 * i:8 * i + 8, cols] for i in range(1, tiles - 1)
                ] + [blank]
                whole, carries[k] = turn_scan(parts, q * VIEWS + k, carries[k])
                for i in range(1, tiles - 1):
                    out[k, 8 * i:8 * i + 8, cols] = whole[8 * i:8 * i + 8]
        return tuple(carries)

    middle = jnp.logical_or(ty == nty // 2, ty == nty // 2 - 1)
    ahead = jnp.where(middle, far, near)
    spread(msg_i, in_i, send_i, recv_i)
    carries = lax.fori_loop(0, ahead, interior, (lowest,) * VIEWS)

    edges = ((top, 0), (bot, ROWS - 8))
    for h in range(2):
        @pl.when(has_down)
        def _():
            halo(0, h, ty + 1).wait_recv()

        @pl.when(has_up)
        def _():
            halo(1, h, ty - 1).wait_recv()

        for k in range(VIEWS):
            for e, (src, row) in enumerate(edges):
                at = 16 * k + 8 * e
                peak = None if h == 0 else bpeaks[64 + at:72 + at, :]
                for c in range(h * half, (h + 1) * half):
                    part = lift(src[h], c - h * half, c, k, 8 + shift[k])
                    sums[k, 8 * e:8 * e + 8, c * LANES:(c + 1) * LANES] = part
                    peak = part if peak is None else jnp.maximum(peak, part)
                if h == 0:
                    firsts[at:at + 8, :] = peak
                at = at + 64 if h == 0 else at
                bpeaks[at:at + 8, :] = peak
    msg_b[...] = jnp.max(bpeaks[...].T, axis=0, keepdims=True)
    spread(msg_b, in_b, send_b, recv_b)

    lax.fori_loop(ahead, chunks // group, interior, carries)

    carry = lowest
    for c in range(half):
        places = [
            (k, e, pl.ds((c + h * half) * LANES, LANES))
            for h in range(2) for k in range(VIEWS) for e in range(2)
        ]
        parts = [sums[k, 8 * e:8 * e + 8, cols] for k, e, cols in places]
        whole, carry = turn_scan(parts, c, carry)
        for n, (k, e, cols) in enumerate(places):
            row = edges[e][1]
            out[k, row:row + 8, cols] = whole[8 * n:8 * n + 8]

    receive(in_i, send_i, recv_i)
    for k in range(VIEWS):
        best = jnp.full((1, LANES), NEG, jnp.float32)
        for p in range(ntx - 1):
            best = jnp.maximum(best, jnp.where(p < tx, in_i[p, k], NEG))
        bsplat_i[k] = jnp.broadcast_to(best, (LANES, LANES)).T

    def close(k, row, before, span):
        for c in span:
            at = (k, pl.ds(row, 8), pl.ds(c * LANES, LANES))
            out[at] = jnp.maximum(out[at], before) - ls[at]

    def close_interior(i, _):
        row = pl.multiple_of(i * 8, 8)
        for k in range(VIEWS):
            close(k, row, bsplat_i[k, pl.ds(row, 8), :], range(chunks))
        return 0

    lax.fori_loop(1, tiles - 1, close_interior, 0)

    @pl.when(has_up)
    def _():
        for h in range(2):
            halo(0, h, ty - 1).wait_send()

    @pl.when(has_down)
    def _():
        for h in range(2):
            halo(1, h, ty + 1).wait_send()

    finish_sends(in_i, send_i, recv_i)
    finish_sends(in_b, send_b, recv_b)

    receive(in_b, send_b, recv_b)
    best = jnp.full((1, LANES), NEG, jnp.float32)
    for p in range(ntx - 1):
        best = jnp.maximum(best, jnp.where(p < tx, in_b[p], NEG))
    before_b[...] = best


def finish(x, sums, before_b, firsts, out, done, inner_sem, edge_sem):
    half = x.shape[2] // LANES // 2
    inner = pltpu.make_async_copy(
        x.at[:, pl.ds(8, ROWS - 16)], out.at[:, pl.ds(8, ROWS - 16)], inner_sem
    )
    inner.start()
    splat = jnp.broadcast_to(before_b[...], (LANES, LANES)).T
    for k in range(VIEWS):
        for e, row in enumerate((0, ROWS - 8)):
            at = 16 * k + 8 * e
            before = splat[at:at + 8, :]
            own = jnp.max(firsts[at:at + 8, :], axis=1, keepdims=True)
            for h, held in enumerate((before, jnp.maximum(before, own))):
                for c in range(h * half, (h + 1) * half):
                    cols = slice(c * LANES, (c + 1) * LANES)
                    run = jnp.maximum(x[k, row:row + 8, cols], held)
                    done[k, 8 * e:8 * e + 8, cols] = run - sums[k, 8 * e:8 * e + 8, cols]
    copies = [
        pltpu.make_async_copy(
            done.at[:, pl.ds(8 * e, 8)], out.at[:, pl.ds(row, 8)], edge_sem.at[e]
        )
        for e, row in enumerate((0, ROWS - 8))
    ]
    for copy in copies:
        copy.start()
    for copy in copies:
        copy.wait()
    inner.wait()


def on_device(surface_levels, bearing_index, stencil_displacements, camera_altitude_class):
    rows, width = surface_levels.shape
    nty, ntx = lax.axis_size("ty"), lax.axis_size("tx")
    chunks = width // LANES
    group, pre, near, far = 4, 5, 1, 2
    vm = lambda *s: pltpu.VMEM(s, jnp.float32)
    dma = pltpu.SemaphoreType.DMA
    arrays = [
        pltpu.with_memory_space_constraint(a, pltpu.HBM)
        for a in (surface_levels, bearing_index, stencil_displacements, camera_altitude_class)
    ]
    parts = pl.pallas_call(
        functools.partial(kernel, nty, ntx, chunks, group, pre, near, far),
        out_shape=[
            jax.ShapeDtypeStruct(shape, jnp.float32)
            for shape in (
                (VIEWS, rows, width), (VIEWS, 16, width), (1, LANES), (LANES // 2, LANES)
            )
        ],
        in_specs=[pl.BlockSpec(memory_space=pltpu.HBM)] * 4,
        out_specs=[pl.BlockSpec(memory_space=pltpu.VMEM)] * 4,
        scratch_shapes=[
            pltpu.SMEM((3, VIEWS), jnp.int32),
            vm(chunks, ROWS, LANES)] + [vm(chunks // 2, 24, LANES)] * 4 + [
            vm(VIEWS, rows, width), vm(VIEWS, 4, 8, LANES), vm(VIEWS, chunks, 8, LANES),
            vm(group * VIEWS, 136, LANES), vm(group * VIEWS, 136, LANES),
            vm(VIEWS, ROWS, LANES), vm(LANES, LANES),
            vm(VIEWS, 1, LANES), vm(1, LANES),
            vm(ntx, VIEWS, 1, LANES), vm(ntx, 1, LANES),
            vm(VIEWS, LANES, LANES),
            dma, dma, dma, dma((3,)),
            dma((2, 2)), dma((2, 2)), dma, dma, dma, dma,
        ],
        compiler_params=pltpu.CompilerParams(
            collective_id=0, has_side_effects=True, vmem_limit_bytes=40 * 1024 * 1024
        ),
        name="horizon",
    )(*arrays)
    return pl.pallas_call(
        finish,
        out_shape=jax.ShapeDtypeStruct((VIEWS, rows, width), jnp.float32),
        in_specs=[pl.BlockSpec(memory_space=pltpu.VMEM)] * 4,
        out_specs=pl.BlockSpec(memory_space=pltpu.HBM),
        scratch_shapes=[vm(VIEWS, 16, width), dma, dma((2,))],
        compiler_params=pltpu.CompilerParams(vmem_limit_bytes=8 * 1024 * 1024),
        name="finish",
    )(*parts)


def solution(mesh):
    return jax.shard_map(
        on_device,
        mesh=mesh,
        in_specs=(P("ty", "tx"), P(), P(), P()),
        out_specs=P(None, "ty", "tx"),
        check_vma=False,
    )
```

```python
import functools
import math

import jax
import jax.numpy as jnp
from jax import lax
from jax.experimental import pallas as pl
from jax.experimental.pallas import tpu as pltpu
from jax.sharding import PartitionSpec as P

VIEWS = 4
ROWS = 128
LANES = 128
NEG = -jnp.inf


def tables(bearing, camera, k, span):
    a = jnp.full((8, LANES), bearing[k], jnp.int32)
    cls = jnp.full((8, LANES), camera[k], jnp.int32).astype(jnp.float32)
    f = (((a * 5) & 15).astype(jnp.float32) + 0.5) / 16.0
    theta = (a.astype(jnp.float32) - 7.5) * (math.pi / 32.0)
    stride = 1.0 / jnp.cos(theta)
    slope = (1.0 + cls) / (4.0 * span)
    cube = f * f * f
    square = f * f
    taps = (
        (-cube + 2.0 * square - f) / 2.0,
        (3.0 * cube - 5.0 * square + 2.0) / 2.0,
        (-3.0 * cube + 4.0 * square + f) / 2.0,
        (cube - square) / 2.0,
    )
    return taps, stride * slope


def sub_scan(total, sub):
    for step in (1, 2, 4):
        total = jnp.maximum(total, jnp.where(sub >= step, pltpu.roll(total, step, 0), NEG))
    return total


def kernel(
    nty, ntx, chunks, group, pre, near, far,
    x_hbm, bearing_hbm, shift_hbm, camera_hbm, out, sums, before_b, firsts,
    tab, xs, top0, top1, bot0, bot1, ls, wv, slants, flat, scan,
    peaks, bpeaks, msg_i, msg_b, in_i, in_b, bsplat_i,
    in_sem, edge_in, tab_sem, halo_send, halo_recv,
    send_i, recv_i, send_b, recv_b,
):
    ty = lax.axis_index("ty")
    tx = lax.axis_index("tx")
    width = chunks * LANES
    span = width * ntx
    tiles = ROWS // 8
    half = chunks // 2
    has_up = ty > 0
    has_down = ty < nty - 1
    mesh_id = pl.DeviceIdType.MESH
    barrier = pltpu.get_barrier_semaphore()
    top, bot = (top0, top1), (bot0, bot1)

    def greet(p):
        pl.semaphore_signal(barrier, inc=1, device_id=p, device_id_type=mesh_id)

    @pl.when(has_up)
    def _():
        greet({"ty": ty - 1, "tx": tx})

    @pl.when(has_down)
    def _():
        greet({"ty": ty + 1, "tx": tx})

    for p in range(ntx - 1):
        @pl.when(p < tx)
        def _():
            greet({"ty": ty, "tx": p})

    for c in range(chunks):
        cols = pl.ds(c * LANES, LANES)
        pltpu.make_async_copy(
            x_hbm.at[pl.ds(0, 16), cols], top[c // half].at[c % half, pl.ds(8, 16)], edge_in
        ).start()
        pltpu.make_async_copy(
            x_hbm.at[pl.ds(ROWS - 16, 16), cols], bot[c // half].at[c % half, pl.ds(0, 16)],
            edge_in,
        ).start()
    small = [
        pltpu.make_async_copy(src, tab.at[n], tab_sem.at[n])
        for n, src in enumerate((bearing_hbm, shift_hbm, camera_hbm))
    ]
    for copy in small:
        copy.start()
    for c in range(chunks):
        pltpu.make_async_copy(
            x_hbm.at[:, pl.ds(c * LANES, LANES)], xs.at[c], in_sem
        ).start()

    blank = jnp.zeros((8, LANES), jnp.float32)
    lowest = jnp.full((8, LANES), NEG, jnp.float32)

    @pl.when(jnp.logical_not(has_up))
    def _():
        for c in range(chunks):
            top[c // half][c % half, 0:8] = blank

    @pl.when(jnp.logical_not(has_down))
    def _():
        for c in range(chunks):
            bot[c // half][c % half, 16:24] = blank

    def arrived(rows, cols, sem):
        pltpu.make_async_copy(
            x_hbm.at[pl.ds(0, rows), pl.ds(0, cols)],
            ls.at[0, pl.ds(0, rows), pl.ds(0, cols)], sem,
        ).wait()

    arrived(32, width, edge_in)

    for copy in small:
        copy.wait()
    bearing, shift, camera = (
        [tab[n, k] for k in range(VIEWS)] for n in range(3)
    )
    lane = lax.broadcasted_iota(jnp.int32, (8, LANES), 1)
    sub = lax.broadcasted_iota(jnp.int32, (8, LANES), 0)
    first = tx * width
    for k in range(VIEWS):
        taps, rise = tables(bearing, camera, k, span)
        for j in range(4):
            wv[k, j] = taps[j]
        for c in range(chunks):
            slants[k, c] = rise * (lane + (first + c * LANES)).astype(jnp.float32)

    for k in range(VIEWS):
        peaks[k, 0:8, :] = lowest
        peaks[k, ROWS - 8:ROWS, :] = lowest

    arrived(ROWS, width, in_sem)

    def lift(src, at, c, k, start):
        acc = wv[k, 0] * src[at, pl.ds(start - 1, 8), :]
        for j in range(1, 4):
            acc = acc + wv[k, j] * src[at, pl.ds(start + j - 1, 8), :]
        return acc + slants[k, c]

    def lift_interior(i, _):
        row = pl.multiple_of(i * 8, 8)
        for k in range(VIEWS):
            peak = None
            for c in range(chunks):
                part = lift(xs, c, c, k, row + shift[k])
                ls[k, pl.ds(row, 8), c * LANES:(c + 1) * LANES] = part
                peak = part if peak is None else jnp.maximum(peak, part)
            peaks[k, pl.ds(row, 8), :] = peak
        return 0

    lax.fori_loop(1, 1 + pre, lift_interior, 0)

    pl.semaphore_wait(
        barrier, (ntx - 1 - tx) + has_up.astype(jnp.int32) + has_down.astype(jnp.int32)
    )

    def halo(n, h, peer):
        if n == 0:
            src, dst = top[h].at[:, pl.ds(8, 6), :], bot[h].at[:, pl.ds(16, 6), :]
        else:
            src, dst = bot[h].at[:, pl.ds(11, 5), :], top[h].at[:, pl.ds(3, 5), :]
        return pltpu.make_async_remote_copy(
            src_ref=src, dst_ref=dst,
            send_sem=halo_send.at[n], recv_sem=halo_recv.at[n, h],
            device_id={"ty": peer, "tx": tx}, device_id_type=mesh_id,
        )

    @pl.when(has_up)
    def _():
        for h in range(2):
            halo(0, h, ty - 1).start()

    @pl.when(has_down)
    def _():
        for h in range(2):
            halo(1, h, ty + 1).start()

    lax.fori_loop(1 + pre, tiles - 1, lift_interior, 0)
    for k in range(VIEWS):
        msg_i[k] = jnp.max(peaks[k].T, axis=0, keepdims=True)

    def spread(msg, store, send, recv):
        for p in list(range(ntx // 2, ntx)) + list(range(1, ntx // 2)):
            @pl.when(p > tx)
            def _():
                pltpu.make_async_remote_copy(
                    src_ref=msg, dst_ref=store.at[tx], send_sem=send, recv_sem=recv,
                    device_id={"ty": ty, "tx": p}, device_id_type=mesh_id,
                ).start()

    def all_of(store, send, recv, n):
        some = store.at[pl.ds(0, n)]
        return pltpu.make_async_remote_copy(
            src_ref=some, dst_ref=some, send_sem=send, recv_sem=recv,
            device_id={"ty": ty, "tx": tx}, device_id_type=mesh_id,
        )

    def all_sent(n, count):
        both = xs.at[:, pl.ds(0, count), :]
        pltpu.make_async_remote_copy(
            src_ref=both, dst_ref=both, send_sem=halo_send.at[n], recv_sem=halo_recv.at[n, 0],
            device_id={"ty": ty, "tx": tx}, device_id_type=mesh_id,
        ).wait_send()

    def finish_sends(store, send, recv):
        for n in range(1, ntx):
            @pl.when(ntx - 1 - tx == n)
            def _():
                all_of(store, send, recv, n).wait_send()

    def receive(store, send, recv):
        for n in range(1, ntx):
            @pl.when(tx == n)
            def _():
                all_of(store, send, recv, n).wait_recv()

    def turn_scan(parts, n, carry):
        turned = jnp.concatenate(parts, axis=0).T
        for t in range(16):
            at = 8 * t + t // 2
            flat[n, at:at + 8, :] = turned[8 * t:8 * t + 8]
        runs = [flat[n, pl.ds(0, 8, stride=17), :]]
        for u in range(1, 16):
            runs.append(jnp.maximum(runs[-1], flat[n, pl.ds(u, 8, stride=17), :]))
        total = sub_scan(runs[-1], sub)
        before = jnp.maximum(jnp.where(sub >= 1, pltpu.roll(total, 1, 0), NEG), carry)
        carry = jnp.maximum(carry, jnp.broadcast_to(total[7:8], (8, LANES)))
        for u in range(16):
            scan[n, pl.ds(u, 8, stride=17), :] = jnp.maximum(runs[u], before)
        whole = jnp.concatenate(
            [scan[n, 8 * t + t // 2:8 * t + t // 2 + 8, :] for t in range(16)], axis=0
        ).T
        return whole, carry

    def interior(g, carries):
        carries = list(carries)
        for q in range(group):
            c = g * group + q
            cols = pl.ds(pl.multiple_of(c * LANES, LANES), LANES)
            for k in range(VIEWS):
                parts = [blank] + [
                    ls[k, 8 * i:8 * i + 8, cols] for i in range(1, tiles - 1)
                ] + [blank]
                whole, carries[k] = turn_scan(parts, q * VIEWS + k, carries[k])
                for i in range(1, tiles - 1):
                    out[k, 8 * i:8 * i + 8, cols] = whole[8 * i:8 * i + 8]
        return tuple(carries)

    middle = jnp.logical_or(ty == nty // 2, ty == nty // 2 - 1)
    ahead = jnp.where(middle, far, near)
    spread(msg_i, in_i, send_i, recv_i)
    carries = lax.fori_loop(0, ahead, interior, (lowest,) * VIEWS)

    edges = ((top, 0), (bot, ROWS - 8))
    for h in range(2):
        @pl.when(has_down)
        def _():
            halo(0, h, ty + 1).wait_recv()

        @pl.when(has_up)
        def _():
            halo(1, h, ty - 1).wait_recv()

        for k in range(VIEWS):
            for e, (src, row) in enumerate(edges):
                at = 16 * k + 8 * e
                peak = None if h == 0 else bpeaks[64 + at:72 + at, :]
                for c in range(h * half, (h + 1) * half):
                    part = lift(src[h], c - h * half, c, k, 8 + shift[k])
                    sums[k, 8 * e:8 * e + 8, c * LANES:(c + 1) * LANES] = part
                    peak = part if peak is None else jnp.maximum(peak, part)
                if h == 0:
                    firsts[at:at + 8, :] = peak
                at = at + 64 if h == 0 else at
                bpeaks[at:at + 8, :] = peak
    msg_b[...] = jnp.max(bpeaks[...].T, axis=0, keepdims=True)
    spread(msg_b, in_b, send_b, recv_b)

    lax.fori_loop(ahead, chunks // group, interior, carries)

    carry = lowest
    for c in range(half):
        places = [
            (k, e, pl.ds((c + h * half) * LANES, LANES))
            for h in range(2) for k in range(VIEWS) for e in range(2)
        ]
        parts = [sums[k, 8 * e:8 * e + 8, cols] for k, e, cols in places]
        whole, carry = turn_scan(parts, c, carry)
        for n, (k, e, cols) in enumerate(places):
            row = edges[e][1]
            out[k, row:row + 8, cols] = whole[8 * n:8 * n + 8]

    receive(in_i, send_i, recv_i)
    for k in range(VIEWS):
        best = jnp.full((1, LANES), NEG, jnp.float32)
        for p in range(ntx - 1):
            best = jnp.maximum(best, jnp.where(p < tx, in_i[p, k], NEG))
        bsplat_i[k] = jnp.broadcast_to(best, (LANES, LANES)).T

    def close(k, row, before, span):
        for c in span:
            at = (k, pl.ds(row, 8), pl.ds(c * LANES, LANES))
            out[at] = jnp.maximum(out[at], before) - ls[at]

    def close_interior(i, _):
        row = pl.multiple_of(i * 8, 8)
        for k in range(VIEWS):
            close(k, row, bsplat_i[k, pl.ds(row, 8), :], range(chunks))
        return 0

    lax.fori_loop(1, tiles - 1, close_interior, 0)

    @pl.when(has_up)
    def _():
        all_sent(0, 6)

    @pl.when(has_down)
    def _():
        all_sent(1, 5)

    finish_sends(in_i, send_i, recv_i)
    finish_sends(in_b, send_b, recv_b)

    receive(in_b, send_b, recv_b)
    best = jnp.full((1, LANES), NEG, jnp.float32)
    for p in range(ntx - 1):
        best = jnp.maximum(best, jnp.where(p < tx, in_b[p], NEG))
    before_b[...] = best


def finish(x, sums, before_b, firsts, out, done, inner_sem, edge_sem):
    half = x.shape[2] // LANES // 2
    inner = pltpu.make_async_copy(
        x.at[:, pl.ds(8, ROWS - 16)], out.at[:, pl.ds(8, ROWS - 16)], inner_sem
    )
    inner.start()
    splat = jnp.broadcast_to(before_b[...], (LANES, LANES)).T
    for k in range(VIEWS):
        for e, row in enumerate((0, ROWS - 8)):
            at = 16 * k + 8 * e
            before = splat[at:at + 8, :]
            own = jnp.max(firsts[at:at + 8, :], axis=1, keepdims=True)
            for h, held in enumerate((before, jnp.maximum(before, own))):
                for c in range(h * half, (h + 1) * half):
                    cols = slice(c * LANES, (c + 1) * LANES)
                    run = jnp.maximum(x[k, row:row + 8, cols], held)
                    done[k, 8 * e:8 * e + 8, cols] = run - sums[k, 8 * e:8 * e + 8, cols]
    copies = [
        pltpu.make_async_copy(
            done.at[:, pl.ds(8 * e, 8)], out.at[:, pl.ds(row, 8)], edge_sem.at[e]
        )
        for e, row in enumerate((0, ROWS - 8))
    ]
    for copy in copies:
        copy.start()
    for copy in copies:
        copy.wait()
    inner.wait()


def on_device(surface_levels, bearing_index, stencil_displacements, camera_altitude_class):
    rows, width = surface_levels.shape
    nty, ntx = lax.axis_size("ty"), lax.axis_size("tx")
    chunks = width // LANES
    group, pre, near, far = 4, 3, 1, 3
    vm = lambda *s: pltpu.VMEM(s, jnp.float32)
    dma = pltpu.SemaphoreType.DMA
    arrays = [
        pltpu.with_memory_space_constraint(a, pltpu.HBM)
        for a in (surface_levels, bearing_index, stencil_displacements, camera_altitude_class)
    ]
    parts = pl.pallas_call(
        functools.partial(kernel, nty, ntx, chunks, group, pre, near, far),
        out_shape=[
            jax.ShapeDtypeStruct(shape, jnp.float32)
            for shape in (
                (VIEWS, rows, width), (VIEWS, 16, width), (1, LANES), (LANES // 2, LANES)
            )
        ],
        in_specs=[pl.BlockSpec(memory_space=pltpu.HBM)] * 4,
        out_specs=[pl.BlockSpec(memory_space=pltpu.VMEM)] * 4,
        scratch_shapes=[
            pltpu.SMEM((3, VIEWS), jnp.int32),
            vm(chunks, ROWS, LANES)] + [vm(chunks // 2, 24, LANES)] * 4 + [
            vm(VIEWS, rows, width), vm(VIEWS, 4, 8, LANES), vm(VIEWS, chunks, 8, LANES),
            vm(group * VIEWS, 136, LANES), vm(group * VIEWS, 136, LANES),
            vm(VIEWS, ROWS, LANES), vm(LANES, LANES),
            vm(VIEWS, 1, LANES), vm(1, LANES),
            vm(ntx, VIEWS, 1, LANES), vm(ntx, 1, LANES),
            vm(VIEWS, LANES, LANES),
            dma, dma, dma((3,)),
            dma((2,)), dma((2, 2)), dma, dma, dma, dma,
        ],
        compiler_params=pltpu.CompilerParams(
            collective_id=0, has_side_effects=True, vmem_limit_bytes=40 * 1024 * 1024
        ),
        name="horizon",
    )(*arrays)
    return pl.pallas_call(
        finish,
        out_shape=jax.ShapeDtypeStruct((VIEWS, rows, width), jnp.float32),
        in_specs=[pl.BlockSpec(memory_space=pltpu.VMEM)] * 4,
        out_specs=pl.BlockSpec(memory_space=pltpu.HBM),
        scratch_shapes=[vm(VIEWS, 16, width), dma, dma((2,))],
        compiler_params=pltpu.CompilerParams(vmem_limit_bytes=8 * 1024 * 1024),
        name="finish",
    )(*parts)


def solution(mesh):
    return jax.shard_map(
        on_device,
        mesh=mesh,
        in_specs=(P("ty", "tx"), P(), P(), P()),
        out_specs=P(None, "ty", "tx"),
        check_vma=False,
    )
```

```python
import functools
import math

import jax
import jax.numpy as jnp
from jax import lax
from jax.experimental import pallas as pl
from jax.experimental.pallas import tpu as pltpu
from jax.sharding import PartitionSpec as P

VIEWS = 4
ROWS = 128
LANES = 128
NEG = -jnp.inf


def tables(bearing, camera, k, span):
    a = jnp.full((8, LANES), bearing[k], jnp.int32)
    cls = jnp.full((8, LANES), camera[k], jnp.int32).astype(jnp.float32)
    f = (((a * 5) & 15).astype(jnp.float32) + 0.5) / 16.0
    theta = (a.astype(jnp.float32) - 7.5) * (math.pi / 32.0)
    stride = 1.0 / jnp.cos(theta)
    slope = (1.0 + cls) / (4.0 * span)
    cube = f * f * f
    square = f * f
    taps = (
        (-cube + 2.0 * square - f) / 2.0,
        (3.0 * cube - 5.0 * square + 2.0) / 2.0,
        (-3.0 * cube + 4.0 * square + f) / 2.0,
        (cube - square) / 2.0,
    )
    return taps, stride * slope


def sub_scan(total, sub):
    for step in (1, 2, 4):
        total = jnp.maximum(total, jnp.where(sub >= step, pltpu.roll(total, step, 0), NEG))
    return total


def kernel(
    nty, ntx, chunks, group, pre, near, far,
    x_hbm, bearing_hbm, shift_hbm, camera_hbm, out, sums, before_b, firsts,
    tab, xs, top0, top1, bot0, bot1, ls, wv, slants, flat, scan,
    peaks, bpeaks, msg_i, msg_b, in_i, in_b, bsplat_i,
    in_sem, edge_in, tab_sem, halo_recv,
    recv_i, recv_b,
):
    halo_send = (edge_in, in_sem)
    send_i, send_b = tab_sem.at[0], tab_sem.at[1]
    ty = lax.axis_index("ty")
    tx = lax.axis_index("tx")
    width = chunks * LANES
    span = width * ntx
    tiles = ROWS // 8
    half = chunks // 2
    has_up = ty > 0
    has_down = ty < nty - 1
    mesh_id = pl.DeviceIdType.MESH
    barrier = pltpu.get_barrier_semaphore()
    top, bot = (top0, top1), (bot0, bot1)

    def greet(p):
        pl.semaphore_signal(barrier, inc=1, device_id=p, device_id_type=mesh_id)

    @pl.when(has_up)
    def _():
        greet({"ty": ty - 1, "tx": tx})

    @pl.when(has_down)
    def _():
        greet({"ty": ty + 1, "tx": tx})

    for p in range(ntx - 1):
        @pl.when(p < tx)
        def _():
            greet({"ty": ty, "tx": p})

    for c in range(chunks):
        cols = pl.ds(c * LANES, LANES)
        pltpu.make_async_copy(
            x_hbm.at[pl.ds(0, 16), cols], top[c // half].at[c % half, pl.ds(8, 16)], edge_in
        ).start()
        pltpu.make_async_copy(
            x_hbm.at[pl.ds(ROWS - 16, 16), cols], bot[c // half].at[c % half, pl.ds(0, 16)],
            edge_in,
        ).start()
    small = [
        pltpu.make_async_copy(src, tab.at[n], tab_sem.at[n])
        for n, src in enumerate((bearing_hbm, shift_hbm, camera_hbm))
    ]
    for copy in small:
        copy.start()
    for c in range(chunks):
        pltpu.make_async_copy(
            x_hbm.at[:, pl.ds(c * LANES, LANES)], xs.at[c], in_sem
        ).start()

    blank = jnp.zeros((8, LANES), jnp.float32)
    lowest = jnp.full((8, LANES), NEG, jnp.float32)

    @pl.when(jnp.logical_not(has_up))
    def _():
        for c in range(chunks):
            top[c // half][c % half, 0:8] = blank

    @pl.when(jnp.logical_not(has_down))
    def _():
        for c in range(chunks):
            bot[c // half][c % half, 16:24] = blank

    def arrived(rows, cols, sem):
        pltpu.make_async_copy(
            x_hbm.at[pl.ds(0, rows), pl.ds(0, cols)],
            ls.at[0, pl.ds(0, rows), pl.ds(0, cols)], sem,
        ).wait()

    arrived(32, width, edge_in)

    for copy in small:
        copy.wait()
    bearing, shift, camera = (
        [tab[n, k] for k in range(VIEWS)] for n in range(3)
    )
    lane = lax.broadcasted_iota(jnp.int32, (8, LANES), 1)
    sub = lax.broadcasted_iota(jnp.int32, (8, LANES), 0)
    first = tx * width
    for k in range(VIEWS):
        taps, rise = tables(bearing, camera, k, span)
        for j in range(4):
            wv[k, j] = taps[j]
        for c in range(chunks):
            slants[k, c] = rise * (lane + (first + c * LANES)).astype(jnp.float32)

    for k in range(VIEWS):
        peaks[k, 0:8, :] = lowest
        peaks[k, ROWS - 8:ROWS, :] = lowest

    arrived(ROWS, width, in_sem)

    def lift(src, at, c, k, start):
        acc = wv[k, 0] * src[at, pl.ds(start - 1, 8), :]
        for j in range(1, 4):
            acc = acc + wv[k, j] * src[at, pl.ds(start + j - 1, 8), :]
        return acc + slants[k, c]

    def lift_interior(i, _):
        row = pl.multiple_of(i * 8, 8)
        for k in range(VIEWS):
            peak = None
            for c in range(chunks):
                part = lift(xs, c, c, k, row + shift[k])
                ls[k, pl.ds(row, 8), c * LANES:(c + 1) * LANES] = part
                peak = part if peak is None else jnp.maximum(peak, part)
            peaks[k, pl.ds(row, 8), :] = peak
        return 0

    lax.fori_loop(1, 1 + pre, lift_interior, 0)

    pl.semaphore_wait(
        barrier, (ntx - 1 - tx) + has_up.astype(jnp.int32) + has_down.astype(jnp.int32)
    )

    def halo(n, h, peer):
        if n == 0:
            src, dst = top[h].at[:, pl.ds(8, 6), :], bot[h].at[:, pl.ds(16, 6), :]
        else:
            src, dst = bot[h].at[:, pl.ds(11, 5), :], top[h].at[:, pl.ds(3, 5), :]
        return pltpu.make_async_remote_copy(
            src_ref=src, dst_ref=dst,
            send_sem=halo_send[n], recv_sem=halo_recv.at[n, h],
            device_id={"ty": peer, "tx": tx}, device_id_type=mesh_id,
        )

    @pl.when(has_up)
    def _():
        for h in range(2):
            halo(0, h, ty - 1).start()

    @pl.when(has_down)
    def _():
        for h in range(2):
            halo(1, h, ty + 1).start()

    lax.fori_loop(1 + pre, tiles - 1, lift_interior, 0)
    for k in range(VIEWS):
        msg_i[k] = jnp.max(peaks[k].T, axis=0, keepdims=True)

    def spread(msg, store, send, recv):
        for p in list(range(ntx // 2, ntx)) + list(range(1, ntx // 2)):
            @pl.when(p > tx)
            def _():
                pltpu.make_async_remote_copy(
                    src_ref=msg, dst_ref=store.at[tx], send_sem=send, recv_sem=recv,
                    device_id={"ty": ty, "tx": p}, device_id_type=mesh_id,
                ).start()

    def all_of(store, send, recv, n):
        some = store.at[pl.ds(0, n)]
        return pltpu.make_async_remote_copy(
            src_ref=some, dst_ref=some, send_sem=send, recv_sem=recv,
            device_id={"ty": ty, "tx": tx}, device_id_type=mesh_id,
        )

    def all_sent(n, count):
        both = xs.at[:, pl.ds(0, count), :]
        pltpu.make_async_remote_copy(
            src_ref=both, dst_ref=both, send_sem=halo_send[n], recv_sem=halo_recv.at[n, 0],
            device_id={"ty": ty, "tx": tx}, device_id_type=mesh_id,
        ).wait_send()

    def finish_sends(store, send, recv):
        for n in range(1, ntx):
            @pl.when(ntx - 1 - tx == n)
            def _():
                all_of(store, send, recv, n).wait_send()

    def receive(store, send, recv):
        for n in range(1, ntx):
            @pl.when(tx == n)
            def _():
                all_of(store, send, recv, n).wait_recv()

    def turn_scan(parts, n, carry):
        turned = jnp.concatenate(parts, axis=0).T
        for t in range(16):
            at = 8 * t + t // 2
            flat[n, at:at + 8, :] = turned[8 * t:8 * t + 8]
        runs = [flat[n, pl.ds(0, 8, stride=17), :]]
        for u in range(1, 16):
            runs.append(jnp.maximum(runs[-1], flat[n, pl.ds(u, 8, stride=17), :]))
        total = sub_scan(runs[-1], sub)
        before = jnp.maximum(jnp.where(sub >= 1, pltpu.roll(total, 1, 0), NEG), carry)
        carry = jnp.maximum(carry, jnp.broadcast_to(total[7:8], (8, LANES)))
        for u in range(16):
            scan[n, pl.ds(u, 8, stride=17), :] = jnp.maximum(runs[u], before)
        whole = jnp.concatenate(
            [scan[n, 8 * t + t // 2:8 * t + t // 2 + 8, :] for t in range(16)], axis=0
        ).T
        return whole, carry

    def interior(g, carries):
        carries = list(carries)
        for q in range(group):
            c = g * group + q
            cols = pl.ds(pl.multiple_of(c * LANES, LANES), LANES)
            for k in range(VIEWS):
                parts = [blank] + [
                    ls[k, 8 * i:8 * i + 8, cols] for i in range(1, tiles - 1)
                ] + [blank]
                whole, carries[k] = turn_scan(parts, q * VIEWS + k, carries[k])
                for i in range(1, tiles - 1):
                    out[k, 8 * i:8 * i + 8, cols] = whole[8 * i:8 * i + 8]
        return tuple(carries)

    middle = jnp.logical_or(ty == nty // 2, ty == nty // 2 - 1)
    ahead = jnp.where(middle, far, near)
    spread(msg_i, in_i, send_i, recv_i)
    carries = lax.fori_loop(0, ahead, interior, (lowest,) * VIEWS)

    edges = ((top, 0), (bot, ROWS - 8))
    for h in range(2):
        @pl.when(has_down)
        def _():
            halo(0, h, ty + 1).wait_recv()

        @pl.when(has_up)
        def _():
            halo(1, h, ty - 1).wait_recv()

        for k in range(VIEWS):
            for e, (src, row) in enumerate(edges):
                at = 16 * k + 8 * e
                peak = None if h == 0 else bpeaks[64 + at:72 + at, :]
                for c in range(h * half, (h + 1) * half):
                    part = lift(src[h], c - h * half, c, k, 8 + shift[k])
                    sums[k, 8 * e:8 * e + 8, c * LANES:(c + 1) * LANES] = part
                    peak = part if peak is None else jnp.maximum(peak, part)
                if h == 0:
                    firsts[at:at + 8, :] = peak
                at = at + 64 if h == 0 else at
                bpeaks[at:at + 8, :] = peak
    msg_b[...] = jnp.max(bpeaks[...].T, axis=0, keepdims=True)
    spread(msg_b, in_b, send_b, recv_b)

    lax.fori_loop(ahead, chunks // group, interior, carries)

    carry = lowest
    for c in range(half):
        places = [
            (k, e, pl.ds((c + h * half) * LANES, LANES))
            for h in range(2) for k in range(VIEWS) for e in range(2)
        ]
        parts = [sums[k, 8 * e:8 * e + 8, cols] for k, e, cols in places]
        whole, carry = turn_scan(parts, c, carry)
        for n, (k, e, cols) in enumerate(places):
            row = edges[e][1]
            out[k, row:row + 8, cols] = whole[8 * n:8 * n + 8]

    receive(in_i, send_i, recv_i)
    for k in range(VIEWS):
        best = jnp.full((1, LANES), NEG, jnp.float32)
        for p in range(ntx - 1):
            best = jnp.maximum(best, jnp.where(p < tx, in_i[p, k], NEG))
        bsplat_i[k] = jnp.broadcast_to(best, (LANES, LANES)).T

    def close(k, row, before, span):
        for c in span:
            at = (k, pl.ds(row, 8), pl.ds(c * LANES, LANES))
            out[at] = jnp.maximum(out[at], before) - ls[at]

    def close_interior(i, _):
        row = pl.multiple_of(i * 8, 8)
        for k in range(VIEWS):
            close(k, row, bsplat_i[k, pl.ds(row, 8), :], range(chunks))
        return 0

    lax.fori_loop(1, tiles - 1, close_interior, 0)

    @pl.when(has_up)
    def _():
        all_sent(0, 6)

    @pl.when(has_down)
    def _():
        all_sent(1, 5)

    finish_sends(in_i, send_i, recv_i)
    finish_sends(in_b, send_b, recv_b)

    receive(in_b, send_b, recv_b)
    best = jnp.full((1, LANES), NEG, jnp.float32)
    for p in range(ntx - 1):
        best = jnp.maximum(best, jnp.where(p < tx, in_b[p], NEG))
    before_b[...] = best


def finish(x, sums, before_b, firsts, out, done, inner_sem, edge_sem):
    half = x.shape[2] // LANES // 2
    inner = pltpu.make_async_copy(
        x.at[:, pl.ds(8, ROWS - 16)], out.at[:, pl.ds(8, ROWS - 16)], inner_sem
    )
    inner.start()
    splat = jnp.broadcast_to(before_b[...], (LANES, LANES)).T
    for k in range(VIEWS):
        for e, row in enumerate((0, ROWS - 8)):
            at = 16 * k + 8 * e
            before = splat[at:at + 8, :]
            own = jnp.max(firsts[at:at + 8, :], axis=1, keepdims=True)
            for h, held in enumerate((before, jnp.maximum(before, own))):
                for c in range(h * half, (h + 1) * half):
                    cols = slice(c * LANES, (c + 1) * LANES)
                    run = jnp.maximum(x[k, row:row + 8, cols], held)
                    done[k, 8 * e:8 * e + 8, cols] = run - sums[k, 8 * e:8 * e + 8, cols]
    copies = [
        pltpu.make_async_copy(
            done.at[:, pl.ds(8 * e, 8)], out.at[:, pl.ds(row, 8)], edge_sem.at[e]
        )
        for e, row in enumerate((0, ROWS - 8))
    ]
    for copy in copies:
        copy.start()
    for copy in copies:
        copy.wait()
    inner.wait()


def on_device(surface_levels, bearing_index, stencil_displacements, camera_altitude_class):
    rows, width = surface_levels.shape
    nty, ntx = lax.axis_size("ty"), lax.axis_size("tx")
    chunks = width // LANES
    group, pre, near, far = 4, 3, 1, 3
    vm = lambda *s: pltpu.VMEM(s, jnp.float32)
    dma = pltpu.SemaphoreType.DMA
    arrays = [
        pltpu.with_memory_space_constraint(a, pltpu.HBM)
        for a in (surface_levels, bearing_index, stencil_displacements, camera_altitude_class)
    ]
    parts = pl.pallas_call(
        functools.partial(kernel, nty, ntx, chunks, group, pre, near, far),
        out_shape=[
            jax.ShapeDtypeStruct(shape, jnp.float32)
            for shape in (
                (VIEWS, rows, width), (VIEWS, 16, width), (1, LANES), (LANES // 2, LANES)
            )
        ],
        in_specs=[pl.BlockSpec(memory_space=pltpu.HBM)] * 4,
        out_specs=[pl.BlockSpec(memory_space=pltpu.VMEM)] * 4,
        scratch_shapes=[
            pltpu.SMEM((3, VIEWS), jnp.int32),
            vm(chunks, ROWS, LANES)] + [vm(chunks // 2, 24, LANES)] * 4 + [
            vm(VIEWS, rows, width), vm(VIEWS, 4, 8, LANES), vm(VIEWS, chunks, 8, LANES),
            vm(group * VIEWS, 136, LANES), vm(group * VIEWS, 136, LANES),
            vm(VIEWS, ROWS, LANES), vm(LANES, LANES),
            vm(VIEWS, 1, LANES), vm(1, LANES),
            vm(ntx, VIEWS, 1, LANES), vm(ntx, 1, LANES),
            vm(VIEWS, LANES, LANES),
            dma, dma, dma((3,)),
            dma((2, 2)), dma, dma,
        ],
        compiler_params=pltpu.CompilerParams(
            collective_id=0, has_side_effects=True, vmem_limit_bytes=40 * 1024 * 1024
        ),
        name="horizon",
    )(*arrays)
    return pl.pallas_call(
        finish,
        out_shape=jax.ShapeDtypeStruct((VIEWS, rows, width), jnp.float32),
        in_specs=[pl.BlockSpec(memory_space=pltpu.VMEM)] * 4,
        out_specs=pl.BlockSpec(memory_space=pltpu.HBM),
        scratch_shapes=[vm(VIEWS, 16, width), dma, dma((2,))],
        compiler_params=pltpu.CompilerParams(vmem_limit_bytes=8 * 1024 * 1024),
        name="finish",
    )(*parts)


def solution(mesh):
    return jax.shard_map(
        on_device,
        mesh=mesh,
        in_specs=(P("ty", "tx"), P(), P(), P()),
        out_specs=P(None, "ty", "tx"),
        check_vma=False,
    )
```
